128 devices in a mesh: dp: 1, tp: 16 (over z, y), pp: 8 (over x, core).
Axes of the slice: x: 4, y: 4, z: 4, core: 2. Of those that a mesh axis runs over, the one named last changes fastest.
Arguments:
- x_in: bfloat16 [2, 2, 512, 2560], P(None, 'dp', 'tp')
- ln_params: float32 [8, 4, 2560], P('pp')
- w_q: bfloat16 [8, 2560, 32, 1, 80], P('pp', None, 'tp')
- w_k: bfloat16 [8, 2560, 32, 80], P('pp', None, 'tp')
- w_v: bfloat16 [8, 2560, 32, 80], P('pp', None, 'tp')
- w_o: bfloat16 [8, 32, 1, 80, 2560], P('pp', 'tp')
- w_up: bfloat16 [8, 2560, 10240], P('pp', None, 'tp')
- w_down: bfloat16 [8, 10240, 2560], P('pp', 'tp')
Outputs:
- output: bfloat16 [8, 2, 2, 512, 2560], P('pp', None, 'dp', 'tp')
All inputs are finite; a program needn't handle non-finite values.
Results may differ from the reference program's by a relative error of at most 0.02.
Values are sent between devices in bfloat16 or wider.
A program may use at most 1 GiB of HBM per device.

```python
import jax
import jax.numpy as jnp
from jax import lax

STAGES = 8
MICRO_BATCHES = 2
BATCH_SIZE = 2
SEQ_LEN = 512
D_MODEL = 2560
NUM_HEADS = 32
KV_COUNT = 32
HEAD_DIM = 80
FF_DIM = 10240

GROUP_SIZE = NUM_HEADS // KV_COUNT
LN_EPS = 1e-5
ROPE_BASE = 10000.0


def setup_inputs(seed: int = 0, part: int = 0) -> dict:
    rng_keys = jax.random.split(jax.random.key(seed), 8)
    x_key = jax.random.fold_in(rng_keys[0], part)
    x_in = jax.random.normal(x_key, (MICRO_BATCHES, BATCH_SIZE, SEQ_LEN, D_MODEL), jnp.float32)
    ln_offset = jnp.array([1.0, 0.0, 1.0, 0.0], jnp.float32)[None, :, None]
    ln_params = ln_offset + 0.5 * jax.random.normal(rng_keys[1], (STAGES, 4, D_MODEL), jnp.float32)
    in_scale = D_MODEL ** -0.5
    w_q = (1.25 * in_scale) * jax.random.normal(rng_keys[2], (STAGES, D_MODEL, KV_COUNT, GROUP_SIZE, HEAD_DIM), jnp.float32)
    w_k = (1.25 * in_scale) * jax.random.normal(rng_keys[3], (STAGES, D_MODEL, KV_COUNT, HEAD_DIM), jnp.float32)
    w_v = in_scale * jax.random.normal(rng_keys[4], (STAGES, D_MODEL, KV_COUNT, HEAD_DIM), jnp.float32)
    w_o = (3.0 * (NUM_HEADS * HEAD_DIM) ** -0.5) * jax.random.normal(rng_keys[5], (STAGES, KV_COUNT, GROUP_SIZE, HEAD_DIM, D_MODEL), jnp.float32)
    w_up = in_scale * jax.random.normal(rng_keys[6], (STAGES, D_MODEL, FF_DIM), jnp.float32)
    w_down = (FF_DIM ** -0.5) * jax.random.normal(rng_keys[7], (STAGES, FF_DIM, D_MODEL), jnp.float32)
    return {"x_in": x_in.astype(jnp.bfloat16), "ln_params": ln_params, "w_q": w_q.astype(jnp.bfloat16), "w_k": w_k.astype(jnp.bfloat16), "w_v": w_v.astype(jnp.bfloat16), "w_o": w_o.astype(jnp.bfloat16), "w_up": w_up.astype(jnp.bfloat16), "w_down": w_down.astype(jnp.bfloat16)}


def layer_norm(x_act, ln_gain, ln_bias):
    x_f32 = x_act.astype(jnp.float32)
    row_mean = jnp.mean(x_f32, axis=-1, keepdims=True)
    centred = x_f32 - row_mean
    variance = jnp.mean(centred * centred, axis=-1, keepdims=True)
    return (centred * lax.rsqrt(variance + LN_EPS) * ln_gain + ln_bias).astype(jnp.bfloat16)


def rope_tables():
    positions = jnp.arange(SEQ_LEN, dtype=jnp.float32)
    inv_freq = ROPE_BASE ** (-2.0 * jnp.arange(HEAD_DIM // 2, dtype=jnp.float32) / HEAD_DIM)
    angles = positions[:, None] * inv_freq[None, :]
    return jnp.cos(angles), jnp.sin(angles)


def apply_rope(proj, cos_tab, sin_tab):
    half_dim = HEAD_DIM // 2
    table_shape = (1, SEQ_LEN) + (1,) * (proj.ndim - 3) + (half_dim,)
    cos_bcast = cos_tab.reshape(table_shape)
    sin_bcast = sin_tab.reshape(table_shape)
    first_half = proj[..., :half_dim]
    second_half = proj[..., half_dim:]
    return jnp.concatenate([first_half * cos_bcast - second_half * sin_bcast, second_half * cos_bcast + first_half * sin_bcast], axis=-1)


def parallel_block(x_act, ln_par, w_q, w_k, w_v, w_o, w_up, w_down):
    num_rows = BATCH_SIZE * SEQ_LEN
    h_attn = layer_norm(x_act, ln_par[0], ln_par[1]).reshape(num_rows, D_MODEL)
    h_mlp = layer_norm(x_act, ln_par[2], ln_par[3]).reshape(num_rows, D_MODEL)
    cos_tab, sin_tab = rope_tables()
    q_proj = jnp.dot(h_attn, w_q.reshape(D_MODEL, NUM_HEADS * HEAD_DIM), preferred_element_type=jnp.float32)
    q_proj = apply_rope(q_proj.reshape(BATCH_SIZE, SEQ_LEN, KV_COUNT, GROUP_SIZE, HEAD_DIM), cos_tab, sin_tab).astype(jnp.bfloat16)
    k_proj = jnp.dot(h_attn, w_k.reshape(D_MODEL, KV_COUNT * HEAD_DIM), preferred_element_type=jnp.float32)
    k_proj = apply_rope(k_proj.reshape(BATCH_SIZE, SEQ_LEN, KV_COUNT, HEAD_DIM), cos_tab, sin_tab).astype(jnp.bfloat16)
    v_proj = jnp.dot(h_attn, w_v.reshape(D_MODEL, KV_COUNT * HEAD_DIM), preferred_element_type=jnp.float32).astype(jnp.bfloat16)
    v_proj = v_proj.reshape(BATCH_SIZE, SEQ_LEN, KV_COUNT, HEAD_DIM)
    allowed = jnp.arange(SEQ_LEN)[:, None, None] >= jnp.arange(SEQ_LEN)[None, None, :]

    def group_attention(operands):
        q_grp, k_grp, v_grp = operands
        scores = jnp.einsum("btgh,bsh->btgs", q_grp.astype(jnp.float32), k_grp.astype(jnp.float32)) * (HEAD_DIM ** -0.5)
        probs_bf = jax.nn.softmax(jnp.where(allowed, scores, -1e30), axis=-1).astype(jnp.bfloat16)
        return jnp.einsum("btgs,bsh->btgh", probs_bf.astype(jnp.float32), v_grp.astype(jnp.float32)).astype(jnp.bfloat16)

    context = lax.map(group_attention, (jnp.moveaxis(q_proj, 2, 0), jnp.moveaxis(k_proj, 2, 0), jnp.moveaxis(v_proj, 2, 0)))
    context = jnp.moveaxis(context, 0, 2).reshape(num_rows, NUM_HEADS * HEAD_DIM)
    attn_out = jnp.dot(context, w_o.reshape(NUM_HEADS * HEAD_DIM, D_MODEL), preferred_element_type=jnp.float32)
    hidden = jax.nn.gelu(jnp.dot(h_mlp, w_up, preferred_element_type=jnp.float32), approximate=False).astype(jnp.bfloat16)
    mlp_out = jnp.dot(hidden, w_down, preferred_element_type=jnp.float32)
    summed = x_act.reshape(num_rows, D_MODEL).astype(jnp.float32) + attn_out + mlp_out
    return summed.astype(jnp.bfloat16).reshape(BATCH_SIZE, SEQ_LEN, D_MODEL)


def reference(x_in, ln_params, w_q, w_k, w_v, w_o, w_up, w_down):
    def one_micro(x_act):
        def stage_step(x_cur, weights):
            ln_par, wq_s, wk_s, wv_s, wo_s, wup_s, wdown_s = weights
            y_next = parallel_block(x_cur, ln_par, wq_s, wk_s, wv_s, wo_s, wup_s, wdown_s)
            return y_next, y_next
        _, per_stage = lax.scan(stage_step, x_act, (ln_params, w_q, w_k, w_v, w_o, w_up, w_down))
        return per_stage
    stacked = lax.map(one_micro, x_in)
    return jnp.swapaxes(stacked, 0, 1)
```

```python
import functools

import jax
import jax.numpy as jnp
import numpy as np
from jax import lax
from jax.experimental import pallas as pl
from jax.experimental.pallas import tpu as pltpu
from jax.sharding import PartitionSpec as P

MESH = pl.DeviceIdType.MESH
LN_EPS = 1e-5
ROPE_BASE = 10000.0
F32, BF16 = jnp.float32, jnp.bfloat16

R = 4
BLK = 32
SEQ = R * R * BLK
D = 2560
HALF = D // 2
HEADS = 2
HD = 80
HH = HD // 2
FF = 640
QKV = 3 * HEADS * HD
ACT = FF + HEADS * HD
CHUNKS = 4


def rope_tables():
    positions = np.arange(SEQ, dtype=np.float32)
    inv_freq = (np.float32(ROPE_BASE) ** (np.float32(-2.0) * np.arange(HH, dtype=np.float32) / np.float32(HD))).astype(np.float32)
    angles = (inv_freq[:, None] * positions[None, :]).astype(np.float32)
    return np.cos(angles).astype(np.float32), np.sin(angles).astype(np.float32)


def nt_dot(a, b):
    return lax.dot_general(a, b, (((1,), (1,)), ((), ())), preferred_element_type=F32)


def nn_dot(a, b):
    return lax.dot_general(a, b, (((1,), (0,)), ((), ())), preferred_element_type=F32)


def kernel(pp_size, x_ref, ln_ref, wq_ref, wk_ref, wv_ref, wo_ref, wup_ref, wdown_ref, cos_ref, sin_ref, out_ref,
           xg, wqkv, wup, wcat, ha, hm, qv, ks, act, part, r1a, r1b, ma, mb, r2a, r2b, ybuf,
           w_sem, in_sem, out_sem, hop_send, hop_recv, g1_send, g1_recv, g2_send, g2_recv,
           s1a_send, s1a_recv, s1b_send, s1b_recv, s2_send, s2_recv):
    tp = lax.axis_index("tp")
    stage = lax.axis_index("pp")
    z, y = lax.div(tp, R), lax.rem(tp, R)
    last = pp_size - 1
    lo, hi = pl.ds(0, HALF), pl.ds(HALF, HALF)

    def row_peer(d):
        return {"tp": z * R + lax.rem(y + d, R)}

    def col_peer(d):
        return {"tp": lax.rem(z + d, R) * R + y}

    def remote(src, dst, send, recv, device):
        return pltpu.make_async_remote_copy(src_ref=src, dst_ref=dst, send_sem=send, recv_sem=recv, device_id=device, device_id_type=MESH)

    barrier = pltpu.get_barrier_semaphore()
    for d in (1, 2, 3):
        pl.semaphore_signal(barrier, inc=1, device_id=row_peer(d), device_id_type=MESH)
        pl.semaphore_signal(barrier, inc=1, device_id=col_peer(d), device_id_type=MESH)

    @pl.when(stage > 0)
    def _():
        pl.semaphore_signal(barrier, inc=1, device_id={"pp": stage - 1}, device_id_type=MESH)

    @pl.when(stage < last)
    def _():
        pl.semaphore_signal(barrier, inc=1, device_id={"pp": stage + 1}, device_id_type=MESH)

    nqk = HEADS * HD
    weight_copies = [
        pltpu.make_async_copy(wq_ref, wqkv.at[pl.ds(0, nqk)], w_sem.at[0]),
        pltpu.make_async_copy(wk_ref, wqkv.at[pl.ds(nqk, nqk)], w_sem.at[1]),
        pltpu.make_async_copy(wv_ref, wqkv.at[pl.ds(2 * nqk, nqk)], w_sem.at[2]),
        pltpu.make_async_copy(wup_ref, wup, w_sem.at[3]),
        pltpu.make_async_copy(wdown_ref, wcat.at[pl.ds(0, FF)], w_sem.at[4]),
        pltpu.make_async_copy(wo_ref, wcat.at[pl.ds(FF, nqk)], w_sem.at[5]),
    ]

    def input_copy(c):
        return pltpu.make_async_copy(x_ref.at[lax.div(c, 2), lax.rem(c, 2)], xg.at[c, z, y], in_sem.at[c])

    @pl.when(stage == 0)
    def _():
        for c in range(CHUNKS):
            input_copy(c).start()

    for cp in weight_copies:
        cp.start()

    pl.semaphore_wait(barrier, 6 + jnp.where(stage > 0, 1, 0) + jnp.where(stage < last, 1, 0))

    def hop_copy(c):
        return remote(ybuf.at[c], xg.at[c, z, y], hop_send.at[c], hop_recv.at[c], {"pp": lax.rem(stage + 1, pp_size)})

    def out_copy(c):
        return pltpu.make_async_copy(ybuf.at[c], out_ref.at[lax.div(c, 2), lax.rem(c, 2)], out_sem.at[c])

    def gather1(c, h, d, zz, yy):
        view = xg.at[c, zz, yy, :, lo if h == 0 else hi]
        return remote(view, view, g1_send.at[h, d - 1], g1_recv.at[c, h, d - 1], row_peer(d) if h == 0 else col_peer(d))

    def gather2(c, h, d, k):
        view = xg.at[c, k, :, :, lo] if h == 0 else xg.at[c, :, k, :, hi]
        return remote(view, view, g2_send.at[h, d - 1], g2_recv.at[c, h, d - 1], col_peer(d) if h == 0 else row_peer(d))

    def scatter1a(c, d):
        return remote(part.at[lax.rem(z + d, R), :, :, lo], r1a.at[c, d - 1], s1a_send.at[d - 1], s1a_recv.at[c, d - 1], col_peer(d))

    def scatter1b(c, e, zz):
        return remote(part.at[zz, lax.rem(y + e, R), :, hi], r1b.at[c, e - 1, zz], s1b_send.at[e - 1, zz], s1b_recv.at[c, e - 1, zz], row_peer(e))

    def scatter2(c, h, d):
        if h == 0:
            return remote(ma.at[lax.rem(y + d, R)], r2a.at[c, d - 1], s2_send.at[0, d - 1], s2_recv.at[c, 0, d - 1], row_peer(d))
        return remote(mb.at[lax.rem(z + d, R)], r2b.at[c, d - 1], s2_send.at[1, d - 1], s2_recv.at[c, 1, d - 1], col_peer(d))

    def back(k, d):
        return lax.rem(k + R - d, R)

    def chunk(c, carry):
        @pl.when(stage == 0)
        def _():
            input_copy(c).wait()

        @pl.when(stage > 0)
        def _():
            hop_copy(c).wait_recv()

        for d in (2, 1, 3):
            gather1(c, 0, d, z, y).start()
            gather1(c, 1, d, z, y).start()
        for d in (1, 2, 3):
            gather1(c, 0, d, z, back(y, d)).wait_recv()
        for d in (2, 1, 3):
            gather2(c, 0, d, z).start()
        for d in (1, 2, 3):
            gather1(c, 1, d, back(z, d), y).wait_recv()
        for d in (2, 1, 3):
            gather2(c, 1, d, y).start()
        for d in (1, 2, 3):
            gather2(c, 0, d, back(z, d)).wait_recv()
            gather2(c, 1, d, back(y, d)).wait_recv()

        def norm(j, carry):
            for half in range(2):
                rows = pl.ds(half * 16, 16)
                x = xg[c, lax.div(j, R), lax.rem(j, R), rows, :].astype(F32)
                mean = jnp.sum(x, axis=-1, keepdims=True) * (1.0 / D)
                x = x - mean
                var = jnp.sum(x * x, axis=-1, keepdims=True) * (1.0 / D)
                x = x * lax.rsqrt(var + LN_EPS)
                dst = pl.ds(pl.multiple_of(j * BLK + half * 16, 16), 16)
                ha[dst, :] = (x * ln_ref[0:1, :] + ln_ref[1:2, :]).astype(BF16)
                hm[dst, :] = (x * ln_ref[2:3, :] + ln_ref[3:4, :]).astype(BF16)
            return carry

        lax.fori_loop(0, R * R, norm, 0)

        @pl.when(c == 0)
        def _():
            for cp in weight_copies:
                cp.wait()

        for tb in range(2):
            toks = pl.ds(tb * 256, 256)
            proj = nt_dot(wqkv[...], ha[toks, :])
            cos, sin = cos_ref[:, toks], sin_ref[:, toks]

            def rope(row):
                first, second = proj[row:row + HH], proj[row + HH:row + HD]
                return jnp.concatenate([first * cos - second * sin, second * cos + first * sin], axis=0)

            for hd in range(HEADS):
                qv[pl.ds(hd * HD, HD), toks] = rope(hd * HD).astype(BF16)
                ks[hd, toks, :] = rope(nqk + hd * HD).T.astype(BF16)
            qv[pl.ds(nqk, nqk), toks] = proj[2 * nqk:].astype(BF16)

        for qb in range(2):
            toks = pl.ds(qb * 256, 256)
            nk = (qb + 1) * 256
            ctx = []
            for hd in range(HEADS):
                scores = nn_dot(ks[hd, 0:nk, :], qv[pl.ds(hd * HD, HD), toks]) * (HD ** -0.5)
                key_pos = lax.broadcasted_iota(jnp.int32, (nk, 256), 0)
                query_pos = lax.broadcasted_iota(jnp.int32, (nk, 256), 1) + qb * 256
                scores = jnp.where(query_pos >= key_pos, scores, -1e30)
                top = jnp.max(scores, axis=0, keepdims=True)
                probs = jnp.exp(scores - top)
                total = jnp.sum(probs, axis=0, keepdims=True)
                probs = (probs * (1.0 / total)).astype(BF16)
                ctx.append(nn_dot(qv[pl.ds(nqk + hd * HD, HD), 0:nk], probs))
            act[toks, FF:ACT] = jnp.concatenate(ctx, axis=0).T.astype(BF16)

        def up(i, carry):
            rows = pl.ds(pl.multiple_of(i * 128, 128), 128)
            pre = nn_dot(hm[rows, :], wup[...])
            act[rows, 0:FF] = (0.5 * pre * (1.0 + lax.erf(pre * np.float32(0.5 ** 0.5)))).astype(BF16)
            return carry

        lax.fori_loop(0, R, up, 0)

        for g in (1, 2, 3, 0):
            zz = lax.rem(z + g, R)
            rows = pl.ds(pl.multiple_of(zz * (R * BLK), R * BLK), R * BLK)
            part[zz] = nn_dot(act[rows, :], wcat[...]).astype(BF16).reshape(R, BLK, D)
            if g:
                scatter1a(c, g).start()
            for e in (2, 1, 3):
                scatter1b(c, e, zz).start()

        for d in (1, 2, 3):
            scatter1a(c, d).wait_recv()
        for d in (2, 1, 3, 0):
            k = lax.rem(y + d, R)
            total = part[z, k, :, lo].astype(F32)
            for e in range(3):
                total += r1a[c, e, k].astype(F32)
            ma[k] = total.astype(BF16)
            if d:
                scatter2(c, 0, d).start()
        for e in (1, 2, 3):
            for k in range(R):
                scatter1b(c, e, k).wait_recv()
        for d in (2, 1, 3, 0):
            k = lax.rem(z + d, R)
            total = part[k, y, :, hi].astype(F32)
            for e in range(3):
                total += r1b[c, e, k].astype(F32)
            mb[k] = total.astype(BF16)
            if d:
                scatter2(c, 1, d).start()
        for d in (1, 2, 3):
            scatter2(c, 0, d).wait_recv()
            scatter2(c, 1, d).wait_recv()
        sum_lo = ma[y].astype(F32)
        sum_hi = mb[z].astype(F32)
        for e in range(3):
            sum_lo += r2a[c, e].astype(F32)
            sum_hi += r2b[c, e].astype(F32)
        ybuf[c, :, lo] = (xg[c, z, y, :, lo].astype(F32) + sum_lo).astype(BF16)
        ybuf[c, :, hi] = (xg[c, z, y, :, hi].astype(F32) + sum_hi).astype(BF16)

        @pl.when(stage < last)
        def _():
            hop_copy(c).start()

        out_copy(c).start()

        for d in (1, 2, 3):
            for h in range(2):
                gather1(c, h, d, z, y).wait_send()
                gather2(c, h, d, z if h == 0 else y).wait_send()
                scatter2(c, h, d).wait_send()
            scatter1a(c, d).wait_send()
            for k in range(R):
                scatter1b(c, d, k).wait_send()
        return carry

    lax.fori_loop(0, CHUNKS, chunk, 0)

    for c in range(CHUNKS):
        out_copy(c).wait()

        @pl.when(stage < last)
        def _():
            hop_copy(c).wait_send()


def solution(mesh):
    pp_size = mesh.shape["pp"]
    cos_tab, sin_tab = rope_tables()
    any_spec = pl.BlockSpec(memory_space=pl.ANY)
    vmem_spec = pl.BlockSpec(memory_space=pltpu.VMEM)
    dma = pltpu.SemaphoreType.DMA

    def body(x_in, ln_params, w_q, w_k, w_v, w_o, w_up, w_down):
        flat = HEADS * HD
        wq = jnp.transpose(w_q[0], (1, 2, 3, 0)).reshape(flat, D)
        wk = jnp.transpose(w_k[0], (1, 2, 0)).reshape(flat, D)
        wv = jnp.transpose(w_v[0], (1, 2, 0)).reshape(flat, D)
        wo = w_o[0].reshape(flat, D)
        out = pl.pallas_call(
            functools.partial(kernel, pp_size),
            out_shape=jax.ShapeDtypeStruct(x_in.shape, BF16),
            in_specs=[any_spec, vmem_spec] + [any_spec] * 6 + [vmem_spec, vmem_spec],
            out_specs=any_spec,
            scratch_shapes=[
                pltpu.VMEM((CHUNKS, R, R, BLK, D), BF16),
                pltpu.VMEM((QKV, D), BF16),
                pltpu.VMEM((D, FF), BF16),
                pltpu.VMEM((ACT, D), BF16),
                pltpu.VMEM((SEQ, D), BF16),
                pltpu.VMEM((SEQ, D), BF16),
                pltpu.VMEM((2 * flat, SEQ), BF16),
                pltpu.VMEM((HEADS, SEQ, HD), BF16),
                pltpu.VMEM((SEQ, ACT), BF16),
                pltpu.VMEM((R, R, BLK, D), BF16),
                pltpu.VMEM((CHUNKS, 3, R, BLK, HALF), BF16),
                pltpu.VMEM((CHUNKS, 3, R, BLK, HALF), BF16),
                pltpu.VMEM((R, BLK, HALF), BF16),
                pltpu.VMEM((R, BLK, HALF), BF16),
                pltpu.VMEM((CHUNKS, 3, BLK, HALF), BF16),
                pltpu.VMEM((CHUNKS, 3, BLK, HALF), BF16),
                pltpu.VMEM((CHUNKS, BLK, D), BF16),
                dma((6,)), dma((CHUNKS,)), dma((CHUNKS,)), dma((CHUNKS,)), dma((CHUNKS,)),
                dma((2, 3)), dma((CHUNKS, 2, 3)), dma((2, 3)), dma((CHUNKS, 2, 3)),
                dma((3,)), dma((CHUNKS, 3)), dma((3, R)), dma((CHUNKS, 3, R)),
                dma((2, 3)), dma((CHUNKS, 2, 3)),
            ],
            compiler_params=pltpu.CompilerParams(collective_id=1, has_side_effects=True, vmem_limit_bytes=62 * 2**20),
            name="pipeline",
        )(x_in, ln_params[0], wq, wk, wv, wo, w_up[0], w_down[0], jnp.asarray(cos_tab), jnp.asarray(sin_tab))
        return out[None]

    in_specs = (P(None, "dp", "tp", None), P("pp", None, None), P("pp", None, "tp", None, None), P("pp", None, "tp", None), P("pp", None, "tp", None), P("pp", "tp", None, None, None), P("pp", None, "tp"), P("pp", "tp", None))
    return jax.shard_map(body, mesh=mesh, in_specs=in_specs, out_specs=P("pp", None, "dp", "tp", None), check_vma=False)
```

```python
import functools

import jax
import jax.numpy as jnp
import numpy as np
from jax import lax
from jax.experimental import pallas as pl
from jax.experimental.pallas import tpu as pltpu
from jax.sharding import PartitionSpec as P

MESH = pl.DeviceIdType.MESH
LN_EPS = 1e-5
ROPE_BASE = 10000.0
F32, BF16 = jnp.float32, jnp.bfloat16

R = 4
BLK = 32
SEQ = R * R * BLK
D = 2560
SUB = BLK // 2
GROUP = R * BLK
ORDER = (0, 1, 3, 2)
SIDE = (0, 1, 1, 0)
HEADS = 2
HD = 80
HH = HD // 2
FF = 640
QKV = 3 * HEADS * HD
ACT = FF + HEADS * HD
CHUNKS = 4


def rope_tables():
    positions = np.arange(SEQ, dtype=np.float32)
    inv_freq = (np.float32(ROPE_BASE) ** (np.float32(-2.0) * np.arange(HH, dtype=np.float32) / np.float32(HD))).astype(np.float32)
    angles = (inv_freq[:, None] * positions[None, :]).astype(np.float32)
    return np.cos(angles).astype(np.float32), np.sin(angles).astype(np.float32)


def nt_dot(a, b):
    return lax.dot_general(a, b, (((1,), (1,)), ((), ())), preferred_element_type=F32)


def nn_dot(a, b):
    return lax.dot_general(a, b, (((1,), (0,)), ((), ())), preferred_element_type=F32)


def kernel(pp_size, x_ref, ln_ref, wq_ref, wk_ref, wv_ref, wo_ref, wup_ref, wdown_ref, cos_ref, sin_ref, out_ref,
           xg, wqkv, wup, wcat, ha, hm, qv, ks, act, part, r1, r2, r3, mid, r4, ybuf,
           w_sem, in_sem, out_sem, hop_send, hop_recv, p1_send, p1_recv, p2_send, p2_recv, p3_send, p3_recv,
           q1_send, q1_recv, q2_send, q2_recv, q3_send, q3_recv):
    tp = lax.axis_index("tp")
    stage = lax.axis_index("pp")
    z, y = lax.div(tp, R), lax.rem(tp, R)
    last = pp_size - 1
    nqk = HEADS * HD

    home = ((z, y), (y, z))

    def at(h, v, u):
        return (v, u) if h == 0 else (u, v)

    def peer(h, dv, du):
        v, u = home[h]
        zz, yy = at(h, lax.rem(v + dv, R), lax.rem(u + du, R))
        return {"tp": zz * R + yy}

    def remote(src, dst, send, recv, device):
        return pltpu.make_async_remote_copy(src_ref=src, dst_ref=dst, send_sem=send, recv_sem=recv, device_id=device, device_id_type=MESH)

    barrier = pltpu.get_barrier_semaphore()
    for d in (1, 2, 3):
        for h in range(2):
            pl.semaphore_signal(barrier, inc=1, device_id=peer(h, 0, d), device_id_type=MESH)

    @pl.when(stage > 0)
    def _():
        pl.semaphore_signal(barrier, inc=1, device_id={"pp": stage - 1}, device_id_type=MESH)

    @pl.when(stage < last)
    def _():
        pl.semaphore_signal(barrier, inc=1, device_id={"pp": stage + 1}, device_id_type=MESH)

    weight_copies = [
        pltpu.make_async_copy(wq_ref, wqkv.at[pl.ds(0, nqk)], w_sem.at[0]),
        pltpu.make_async_copy(wk_ref, wqkv.at[pl.ds(nqk, nqk)], w_sem.at[1]),
        pltpu.make_async_copy(wv_ref, wqkv.at[pl.ds(2 * nqk, nqk)], w_sem.at[2]),
        pltpu.make_async_copy(wup_ref, wup, w_sem.at[3]),
        pltpu.make_async_copy(wdown_ref, wcat.at[pl.ds(0, FF)], w_sem.at[4]),
        pltpu.make_async_copy(wo_ref, wcat.at[pl.ds(FF, nqk)], w_sem.at[5]),
    ]

    def input_copy(c):
        return pltpu.make_async_copy(x_ref.at[lax.div(c, 2), lax.rem(c, 2)], xg.at[c, z, y], in_sem.at[c])

    @pl.when(stage == 0)
    def _():
        for c in range(CHUNKS):
            input_copy(c).start()

    for cp in weight_copies:
        cp.start()

    pl.semaphore_wait(barrier, 6 + jnp.where(stage > 0, 1, 0) + jnp.where(stage < last, 1, 0))

    def hop_copy(c):
        return remote(ybuf.at[c], xg.at[c, z, y], hop_send.at[c], hop_recv.at[c], {"pp": lax.rem(stage + 1, pp_size)})

    def out_copy(c):
        return pltpu.make_async_copy(ybuf.at[c], out_ref.at[lax.div(c, 2), lax.rem(c, 2)], out_sem.at[c])

    def place(h, dv, du):
        v, u = home[h]
        return at(h, lax.rem(v + dv + R, R), lax.rem(u + du + R, R))

    def gathered(c, h, dv, du):
        zz, yy = place(h, dv, du)
        return xg.at[c, zz, yy, pl.ds(h * SUB, SUB), :]

    def partial_at(h, dv, du):
        zz, yy = place(h, dv, du)
        return part.at[zz, yy, pl.ds(h * SUB, SUB), :]

    def p1(c, h, d, incoming=False):
        view = gathered(c, h, 0, -d if incoming else 0)
        return remote(view, view, p1_send.at[h, d - 1], p1_recv.at[c, h, d - 1], peer(h, 0, d))

    def p2(c, h, side, k, incoming=False):
        view = gathered(c, h, ((-1, 1)[side] if incoming else 0), -k)
        return remote(view, view, p2_send.at[h, side, k], p2_recv.at[c, h, side, k], peer(h, (1, R - 1)[side], 0))

    def p3(c, h, k, incoming=False):
        side = SIDE[k]
        view = gathered(c, h, (2 if incoming else (-1, 1)[side]), -k)
        return remote(view, view, p3_send.at[h, k], p3_recv.at[c, h, k], peer(h, (1, R - 1)[side], 0))

    def q1(c, h, k):
        return remote(partial_at(h, 2, -k), r1.at[c, h, k], q1_send.at[h, k], q1_recv.at[c, h, k], peer(h, (1, R - 1)[SIDE[k]], 0))

    def q2(c, h, side, k):
        return remote(partial_at(h, (1, -1)[side], -k), (r2 if side == 0 else r3).at[c, h, k], q2_send.at[h, side, k], q2_recv.at[c, h, side, k],
                      peer(h, (1, R - 1)[side], 0))

    def q3(c, h, k):
        return remote(mid.at[h, k], r4.at[c, h, k - 1], q3_send.at[h, k - 1], q3_recv.at[c, h, k - 1], peer(h, 0, R - k))

    def row_group(c, off):
        zz = lax.rem(z + off, R)
        base = pl.multiple_of(zz * GROUP, GROUP)
        toks = pl.ds(base, GROUP)

        def norm(j, carry):
            x = xg[c, zz, lax.div(j, 2), pl.ds(pl.multiple_of(lax.rem(j, 2) * SUB, SUB), SUB), :].astype(F32)
            mean = jnp.sum(x, axis=-1, keepdims=True) * (1.0 / D)
            x = x - mean
            var = jnp.sum(x * x, axis=-1, keepdims=True) * (1.0 / D)
            x = x * lax.rsqrt(var + LN_EPS)
            dst = pl.ds(pl.multiple_of(j * SUB, SUB), SUB)
            ha[dst, :] = (x * ln_ref[0:1, :] + ln_ref[1:2, :]).astype(BF16)
            hm[dst, :] = (x * ln_ref[2:3, :] + ln_ref[3:4, :]).astype(BF16)
            return carry

        lax.fori_loop(0, GROUP // SUB, norm, 0)

        if off == 0:
            @pl.when(c == 0)
            def _():
                for cp in weight_copies:
                    cp.wait()

        proj = nt_dot(wqkv[...], ha[...])
        cos, sin = cos_ref[:, toks], sin_ref[:, toks]

        def rope(row):
            first, second = proj[row:row + HH], proj[row + HH:row + HD]
            return jnp.concatenate([first * cos - second * sin, second * cos + first * sin], axis=0)

        for hd in range(HEADS):
            qv[pl.ds(hd * HD, HD), toks] = rope(hd * HD).astype(BF16)
            ks[hd, toks, :] = rope(nqk + hd * HD).T.astype(BF16)
        qv[pl.ds(nqk, nqk), toks] = proj[2 * nqk:].astype(BF16)

        pre = nn_dot(hm[...], wup[...])
        act[toks, 0:FF] = (0.5 * pre * (1.0 + lax.erf(pre * np.float32(0.5 ** 0.5)))).astype(BF16)

    def chunk(c, carry):
        @pl.when(stage == 0)
        def _():
            input_copy(c).wait()

        @pl.when(stage > 0)
        def _():
            hop_copy(c).wait_recv()

        for d in (1, 3, 2):
            for h in range(2):
                p1(c, h, d).start()
        for h in range(2):
            for side in range(2):
                p2(c, h, side, 0).start()
        for k in ORDER[1:]:
            for h in range(2):
                p1(c, h, k, True).wait_recv()
                for side in range(2):
                    p2(c, h, side, k).start()

        def forward(k):
            for h in range(2):
                p2(c, h, SIDE[k], k, True).wait_recv()
                p3(c, h, k).start()

        def others(h, side, ks_):
            for k in ks_:
                p2(c, h, side, k, True).wait_recv()

        forward(0)
        forward(1)
        others(1, 1, (0,))
        p3(c, 1, 0, True).wait_recv()
        row_group(c, 0)
        forward(3)
        forward(2)
        others(0, 0, (1, 2))
        others(1, 0, (1,))
        p3(c, 1, 1, True).wait_recv()
        row_group(c, 3)
        others(0, 1, (0, 3))
        others(1, 1, (3,))
        p3(c, 1, 3, True).wait_recv()
        row_group(c, 1)
        for k in ORDER:
            p3(c, 0, k, True).wait_recv()
        others(1, 0, (2,))
        p3(c, 1, 2, True).wait_recv()
        row_group(c, 2)

        for qb in range(2):
            toks = pl.ds(qb * 256, 256)
            nk = (qb + 1) * 256
            ctx = []
            for hd in range(HEADS):
                scores = nn_dot(ks[hd, 0:nk, :], qv[pl.ds(hd * HD, HD), toks]) * (HD ** -0.5)
                key_pos = lax.broadcasted_iota(jnp.int32, (nk, 256), 0)
                query_pos = lax.broadcasted_iota(jnp.int32, (nk, 256), 1) + qb * 256
                scores = jnp.where(query_pos >= key_pos, scores, -1e30)
                top = jnp.max(scores, axis=0, keepdims=True)
                probs = jnp.exp(scores - top)
                total = jnp.sum(probs, axis=0, keepdims=True)
                probs = (probs * (1.0 / total)).astype(BF16)
                ctx.append(nn_dot(qv[pl.ds(nqk + hd * HD, HD), 0:nk], probs))
            act[toks, FF:ACT] = jnp.concatenate(ctx, axis=0).T.astype(BF16)

        for off in (2, 3, 1, 0):
            zz = lax.rem(z + off, R)
            rows = pl.ds(pl.multiple_of(zz * GROUP, GROUP), GROUP)
            part[zz] = nn_dot(act[rows, :], wcat[...]).astype(BF16).reshape(R, BLK, D)
            k1 = (R - off) % R
            q1(c, 1, k1).start()
            if off == 2:
                for k in ORDER:
                    q1(c, 0, k).start()
            elif off == 3:
                for k in ORDER:
                    if SIDE[k] == 0:
                        q2(c, 0, 1, k).start()
            elif off == 1:
                for k in ORDER:
                    if SIDE[k] == 1:
                        q2(c, 0, 0, k).start()
            q2(c, 1, 1 - SIDE[k1], k1).start()

        for h, k in [(0, 0), (0, 1), (1, 2), (0, 3), (0, 2), (1, 1), (1, 3), (1, 0)]:
            side = SIDE[k]
            q1(c, h, k).wait_recv()
            mine = partial_at(h, (1, -1)[side], -k)
            mine[...] = (mine[...].astype(F32) + r1[c, h, k].astype(F32)).astype(BF16)
            q2(c, h, side, k).start()
        for k in (1, 2, 3, 0):
            for h in range(2):
                q2(c, h, 0, k).wait_recv()
                q2(c, h, 1, k).wait_recv()
                total = partial_at(h, 0, -k)[...].astype(F32) + r2[c, h, k].astype(F32) + r3[c, h, k].astype(F32)
                mid[h, k] = total.astype(BF16)
                if k:
                    q3(c, h, k).start()
        for h in range(2):
            rows = pl.ds(h * SUB, SUB)
            total = xg[c, z, y, rows, :].astype(F32) + mid[h, 0].astype(F32)
            for k in (1, 2, 3):
                q3(c, h, k).wait_recv()
                total += r4[c, h, k - 1].astype(F32)
            ybuf[c, rows, :] = total.astype(BF16)

        @pl.when(stage < last)
        def _():
            hop_copy(c).start()

        out_copy(c).start()

        for h in range(2):
            for k in range(R):
                if k:
                    p1(c, h, k).wait_send()
                    q3(c, h, k).wait_send()
                for side in range(2):
                    p2(c, h, side, k).wait_send()
                    q2(c, h, side, k).wait_send()
                p3(c, h, k).wait_send()
                q1(c, h, k).wait_send()
        return carry

    lax.fori_loop(0, CHUNKS, chunk, 0)

    for c in range(CHUNKS):
        out_copy(c).wait()

        @pl.when(stage < last)
        def _():
            hop_copy(c).wait_send()


def solution(mesh):
    pp_size = mesh.shape["pp"]
    cos_tab, sin_tab = rope_tables()
    any_spec = pl.BlockSpec(memory_space=pl.ANY)
    vmem_spec = pl.BlockSpec(memory_space=pltpu.VMEM)
    dma = pltpu.SemaphoreType.DMA

    def body(x_in, ln_params, w_q, w_k, w_v, w_o, w_up, w_down):
        flat = HEADS * HD
        wq = jnp.transpose(w_q[0], (1, 2, 3, 0)).reshape(flat, D)
        wk = jnp.transpose(w_k[0], (1, 2, 0)).reshape(flat, D)
        wv = jnp.transpose(w_v[0], (1, 2, 0)).reshape(flat, D)
        wo = w_o[0].reshape(flat, D)
        out = pl.pallas_call(
            functools.partial(kernel, pp_size),
            out_shape=jax.ShapeDtypeStruct(x_in.shape, BF16),
            in_specs=[any_spec, vmem_spec] + [any_spec] * 6 + [vmem_spec, vmem_spec],
            out_specs=any_spec,
            scratch_shapes=[
                pltpu.VMEM((CHUNKS, R, R, BLK, D), BF16),
                pltpu.VMEM((QKV, D), BF16),
                pltpu.VMEM((D, FF), BF16),
                pltpu.VMEM((ACT, D), BF16),
                pltpu.VMEM((GROUP, D), BF16),
                pltpu.VMEM((GROUP, D), BF16),
                pltpu.VMEM((2 * flat, SEQ), BF16),
                pltpu.VMEM((HEADS, SEQ, HD), BF16),
                pltpu.VMEM((SEQ, ACT), BF16),
                pltpu.VMEM((R, R, BLK, D), BF16),
                pltpu.VMEM((CHUNKS, 2, R, SUB, D), BF16),
                pltpu.VMEM((CHUNKS, 2, R, SUB, D), BF16),
                pltpu.VMEM((CHUNKS, 2, R, SUB, D), BF16),
                pltpu.VMEM((2, R, SUB, D), BF16),
                pltpu.VMEM((CHUNKS, 2, R - 1, SUB, D), BF16),
                pltpu.VMEM((CHUNKS, BLK, D), BF16),
                dma((6,)), dma((CHUNKS,)), dma((CHUNKS,)), dma((CHUNKS,)), dma((CHUNKS,)),
                dma((2, 3)), dma((CHUNKS, 2, 3)), dma((2, 2, R)), dma((CHUNKS, 2, 2, R)), dma((2, R)), dma((CHUNKS, 2, R)),
                dma((2, R)), dma((CHUNKS, 2, R)), dma((2, 2, R)), dma((CHUNKS, 2, 2, R)), dma((2, 3)), dma((CHUNKS, 2, 3)),
            ],
            compiler_params=pltpu.CompilerParams(collective_id=1, has_side_effects=True, vmem_limit_bytes=62 * 2**20),
            name="pipeline",
        )(x_in, ln_params[0], wq, wk, wv, wo, w_up[0], w_down[0], jnp.asarray(cos_tab), jnp.asarray(sin_tab))
        return out[None]

    in_specs = (P(None, "dp", "tp", None), P("pp", None, None), P("pp", None, "tp", None, None), P("pp", None, "tp", None), P("pp", None, "tp", None), P("pp", "tp", None, None, None), P("pp", None, "tp"), P("pp", "tp", None))
    return jax.shard_map(body, mesh=mesh, in_specs=in_specs, out_specs=P("pp", None, "dp", "tp", None), check_vma=False)
```

```python
import functools

import jax
import jax.numpy as jnp
import numpy as np
from jax import lax
from jax.experimental import pallas as pl
from jax.experimental.pallas import tpu as pltpu
from jax.sharding import PartitionSpec as P

MESH = pl.DeviceIdType.MESH
LN_EPS = 1e-5
ROPE_BASE = 10000.0
F32, BF16 = jnp.float32, jnp.bfloat16

R = 4
BLK = 32
SEQ = R * R * BLK
D = 2560
SUB = BLK // 2
GROUP = R * BLK
ORDER = (0, 1, 3, 2)
SIDE = (0, 1, 1, 0)
HEADS = 2
HD = 80
HH = HD // 2
FF = 640
QKV = 3 * HEADS * HD
ACT = FF + HEADS * HD
CHUNKS = 4


def rope_tables():
    positions = np.arange(SEQ, dtype=np.float32)
    inv_freq = (np.float32(ROPE_BASE) ** (np.float32(-2.0) * np.arange(HH, dtype=np.float32) / np.float32(HD))).astype(np.float32)
    angles = (inv_freq[:, None] * positions[None, :]).astype(np.float32)
    return np.cos(angles).astype(np.float32), np.sin(angles).astype(np.float32)


def nt_dot(a, b):
    return lax.dot_general(a, b, (((1,), (1,)), ((), ())), preferred_element_type=F32)


def nn_dot(a, b):
    return lax.dot_general(a, b, (((1,), (0,)), ((), ())), preferred_element_type=F32)


def kernel(pp_size, x_ref, ln_ref, wq_ref, wk_ref, wv_ref, wo_ref, wup_ref, wdown_ref, cos_ref, sin_ref, out_ref,
           xg, wqkv, wup, wcat, ha, hm, qv, ks, act, part, r1, r2, r3, mid, r4, ybuf,
           w_sem, in_sem, out_sem, hop_send, hop_recv, p1_send, p1_recv, p2_send, p2_recv, p3_send, p3_recv,
           q1_send, q1_recv, q2_send, q2_recv, q3_send, q3_recv, turn_sem):
    tp = lax.axis_index("tp")
    stage = lax.axis_index("pp")
    z, y = lax.div(tp, R), lax.rem(tp, R)
    last = pp_size - 1
    nqk = HEADS * HD

    home = ((z, y), (y, z))

    def at(h, v, u):
        return (v, u) if h == 0 else (u, v)

    def peer(h, dv, du):
        v, u = home[h]
        zz, yy = at(h, lax.rem(v + dv, R), lax.rem(u + du, R))
        return {"tp": zz * R + yy}

    def remote(src, dst, send, recv, device):
        return pltpu.make_async_remote_copy(src_ref=src, dst_ref=dst, send_sem=send, recv_sem=recv, device_id=device, device_id_type=MESH)

    barrier = pltpu.get_barrier_semaphore()
    for d in (1, 2, 3):
        for h in range(2):
            pl.semaphore_signal(barrier, inc=1, device_id=peer(h, 0, d), device_id_type=MESH)

    @pl.when(stage > 0)
    def _():
        pl.semaphore_signal(barrier, inc=1, device_id={"pp": stage - 1}, device_id_type=MESH)

    @pl.when(stage < last)
    def _():
        pl.semaphore_signal(barrier, inc=1, device_id={"pp": stage + 1}, device_id_type=MESH)

    weight_copies = [
        pltpu.make_async_copy(wq_ref, wqkv.at[pl.ds(0, nqk)], w_sem.at[0]),
        pltpu.make_async_copy(wk_ref, wqkv.at[pl.ds(nqk, nqk)], w_sem.at[1]),
        pltpu.make_async_copy(wv_ref, wqkv.at[pl.ds(2 * nqk, nqk)], w_sem.at[2]),
        pltpu.make_async_copy(wup_ref, wup, w_sem.at[3]),
        pltpu.make_async_copy(wdown_ref, wcat.at[pl.ds(0, FF)], w_sem.at[4]),
        pltpu.make_async_copy(wo_ref, wcat.at[pl.ds(FF, nqk)], w_sem.at[5]),
    ]

    def input_copy(c):
        return pltpu.make_async_copy(x_ref.at[lax.div(c, 2), lax.rem(c, 2)], xg.at[c, z, y], in_sem.at[c])

    @pl.when(stage == 0)
    def _():
        for c in range(CHUNKS):
            input_copy(c).start()

    for cp in weight_copies:
        cp.start()

    pl.semaphore_wait(barrier, 6 + jnp.where(stage > 0, 1, 0) + jnp.where(stage < last, 1, 0))

    def hop_copy(c):
        return remote(ybuf.at[c], xg.at[c, z, y], hop_send.at[c], hop_recv.at[c], {"pp": lax.rem(stage + 1, pp_size)})

    def out_copy(c):
        return pltpu.make_async_copy(ybuf.at[c], out_ref.at[lax.div(c, 2), lax.rem(c, 2)], out_sem.at[c])

    def place(h, dv, du):
        v, u = home[h]
        return at(h, lax.rem(v + dv + R, R), lax.rem(u + du + R, R))

    def gathered(c, h, dv, du):
        zz, yy = place(h, dv, du)
        return xg.at[c, zz, yy, pl.ds(h * SUB, SUB), :]

    def partial_at(h, dv, du):
        zz, yy = place(h, dv, du)
        return part.at[zz, yy, pl.ds(h * SUB, SUB), :]

    def p1(c, h, d, incoming=False):
        view = gathered(c, h, 0, -d if incoming else 0)
        return remote(view, view, p1_send.at[h, d - 1], p1_recv.at[c, h, d - 1], peer(h, 0, d))

    def p2(c, h, side, k, incoming=False):
        view = gathered(c, h, ((-1, 1)[side] if incoming else 0), -k)
        return remote(view, view, p2_send.at[h, side, k], p2_recv.at[c, h, side, k], peer(h, (1, R - 1)[side], 0))

    def p3(c, h, k, incoming=False):
        side = SIDE[k]
        view = gathered(c, h, 2 if incoming else (-1, 1)[side] if k else 0, -k)
        return remote(view, view, p3_send.at[h, k], p3_recv.at[c, h, k], peer(h, (1, R - 1)[side] if k else 2, 0))

    def q1(c, h, k):
        return remote(partial_at(h, 2, -k), r1.at[c, h, k], q1_send.at[h, k], q1_recv.at[c, h, k], peer(h, (1, R - 1)[SIDE[k]] if k else 2, 0))

    def q2(c, h, side, k):
        return remote(partial_at(h, (1, -1)[side], -k), (r2 if side == 0 else r3).at[c, h, k], q2_send.at[h, side, k], q2_recv.at[c, h, side, k],
                      peer(h, (1, R - 1)[side], 0))

    def q3(c, h, k):
        return remote(mid.at[h, k], r4.at[c, h, k - 1], q3_send.at[h, k - 1], q3_recv.at[c, h, k - 1], peer(h, 0, R - k))

    def norms(c, off, slot):
        zz = lax.rem(z + off, R)
        for yy in range(R):
            total = jnp.sum(xg[c, zz, yy].astype(F32), axis=-1, keepdims=True)
            mean = total * (1.0 / D)
            dev = xg[c, zz, yy].astype(F32) - mean
            var = jnp.sum(dev * dev, axis=-1, keepdims=True) * (1.0 / D)
            scale = lax.rsqrt(var + LN_EPS)
            unit = (xg[c, zz, yy].astype(F32) - mean) * scale
            dst = pl.ds(slot * GROUP + yy * BLK, BLK)
            ha[dst, :] = (unit * ln_ref[0:1, :] + ln_ref[1:2, :]).astype(BF16)
            hm[dst, :] = (unit * ln_ref[2:3, :] + ln_ref[3:4, :]).astype(BF16)

    def project(offs):
        toks = [pl.ds(pl.multiple_of(lax.rem(z + off, R) * GROUP, GROUP), GROUP) for off in offs]

        proj = nt_dot(wqkv[...], ha[...])
        for slot, tok in enumerate(toks):
            cols = proj[:, slot * GROUP:(slot + 1) * GROUP]
            cos, sin = cos_ref[:, tok], sin_ref[:, tok]

            def rope(row):
                first, second = cols[row:row + HH], cols[row + HH:row + HD]
                return jnp.concatenate([first * cos - second * sin, second * cos + first * sin], axis=0)

            for hd in range(HEADS):
                qv[pl.ds(hd * HD, HD), tok] = rope(hd * HD).astype(BF16)
                ks[hd, tok, :] = rope(nqk + hd * HD).T.astype(BF16)
            qv[pl.ds(nqk, nqk), tok] = cols[2 * nqk:].astype(BF16)

        for slot, tok in enumerate(toks):
            pre = nn_dot(hm[slot * GROUP:(slot + 1) * GROUP, :], wup[...])
            act[tok, 0:FF] = (0.5 * pre * (1.0 + lax.erf(pre * np.float32(0.5 ** 0.5)))).astype(BF16)

    def chunk(c, carry):
        with jax.named_scope("wait_in"):
            @pl.when(stage == 0)
            def _():
                input_copy(c).wait()

            @pl.when(stage > 0)
            def _():
                hop_copy(c).wait_recv()

            @pl.when((c > 0) & (lax.rem(stage, 2) == 0))
            def _():
                pl.semaphore_wait(turn_sem, 1)

        with jax.named_scope("p1_wait"):
            for h in range(2):
                for d in (1, 3):
                    p1(c, h, d).start()
                for side in range(2):
                    p2(c, 1 - h, side, 0).start()
                p1(c, h, 2).start()
                p3(c, 1 - h, 0).start()
            for k in ORDER[1:]:
                for h in range(2):
                    p1(c, h, k, True).wait_recv()
                    for side in range(2):
                        p2(c, h, side, k).start()

        def forward(k):
            for h in range(2):
                p2(c, h, SIDE[k], k, True).wait_recv()
                p3(c, h, k).start()

        def others(h, side, ks_):
            for k in ks_:
                p2(c, h, side, k, True).wait_recv()

        with jax.named_scope("wait_g0"):
            others(1, 0, (0,))
            others(1, 1, (0,))
            p3(c, 1, 0, True).wait_recv()
        with jax.named_scope("norm0"):
            norms(c, 0, 0)
        with jax.named_scope("wait_g3"):
            for k in ORDER[1:]:
                forward(k)
            others(0, 0, (0, 1, 2))
            others(1, 0, (1,))
            p3(c, 1, 1, True).wait_recv()

        @pl.when((c < CHUNKS - 1) & (lax.rem(stage, 2) == 1))
        def _():
            pl.semaphore_signal(turn_sem, inc=1, device_id={"pp": stage - 1}, device_id_type=MESH)

        with jax.named_scope("norm3"):
            norms(c, 3, 1)

        @pl.when(c == 0)
        def _():
            for cp in weight_copies:
                cp.wait()

        with jax.named_scope("proj03"):
            project((0, 3))
        with jax.named_scope("wait_g1"):
            others(0, 1, (0, 3))
            others(1, 1, (3,))
            p3(c, 1, 3, True).wait_recv()
        with jax.named_scope("norm1"):
            norms(c, 1, 0)
        with jax.named_scope("wait_g2"):
            for k in ORDER:
                p3(c, 0, k, True).wait_recv()
            others(1, 0, (2,))
            p3(c, 1, 2, True).wait_recv()
        with jax.named_scope("norm2"):
            norms(c, 2, 1)
        with jax.named_scope("proj12"):
            project((1, 2))

        with jax.named_scope("attn"):
            for qb in range(2):
                toks = pl.ds(qb * 256, 256)
                nk = (qb + 1) * 256
                ctx = []
                for hd in range(HEADS):
                    scores = nn_dot(ks[hd, 0:nk, :], qv[pl.ds(hd * HD, HD), toks]) * (HD ** -0.5)
                    key_pos = lax.broadcasted_iota(jnp.int32, (nk, 256), 0)
                    query_pos = lax.broadcasted_iota(jnp.int32, (nk, 256), 1) + qb * 256
                    scores = jnp.where(query_pos >= key_pos, scores, -1e30)
                    top = jnp.max(scores, axis=0, keepdims=True)
                    probs = jnp.exp(scores - top)
                    total = jnp.sum(probs, axis=0, keepdims=True)
                    probs = (probs * (1.0 / total)).astype(BF16)
                    ctx.append(nn_dot(qv[pl.ds(nqk + hd * HD, HD), 0:nk], probs))
                act[toks, FF:ACT] = jnp.concatenate(ctx, axis=0).T.astype(BF16)

        with jax.named_scope("down"):
            for off in (2, 3, 1, 0):
                zz = lax.rem(z + off, R)
                rows = pl.ds(pl.multiple_of(zz * GROUP, GROUP), GROUP)
                part[zz] = nn_dot(act[rows, :], wcat[...]).astype(BF16).reshape(R, BLK, D)
                k1 = (R - off) % R
                q1(c, 1, k1).start()
                for k in ORDER:
                    if off == 2:
                        q1(c, 0, k).start()
                    elif off == 3 and (k == 0 or SIDE[k] == 0):
                        q2(c, 0, 1, k).start()
                    elif off == 1 and (k == 0 or SIDE[k] == 1):
                        q2(c, 0, 0, k).start()
                for side in range(2):
                    if k1 == 0 or SIDE[k1] != side:
                        q2(c, 1, side, k1).start()

        with jax.named_scope("rs_add"):
            for h, k in [(0, 1), (0, 3), (0, 2), (1, 2), (1, 1), (1, 3)]:
                side = SIDE[k]
                q1(c, h, k).wait_recv()
                mine = partial_at(h, (1, -1)[side], -k)
                mine[...] = (mine[...].astype(F32) + r1[c, h, k].astype(F32)).astype(BF16)
                q2(c, h, side, k).start()
        with jax.named_scope("rs_mid"):
            for h, k in [(0, 1), (0, 3), (0, 2), (1, 2), (1, 1), (1, 3), (0, 0), (1, 0)]:
                q2(c, h, 0, k).wait_recv()
                q2(c, h, 1, k).wait_recv()
                total = partial_at(h, 0, -k)[...].astype(F32) + r2[c, h, k].astype(F32) + r3[c, h, k].astype(F32)
                if k == 0:
                    q1(c, h, 0).wait_recv()
                    total += r1[c, h, 0].astype(F32)
                mid[h, k] = total.astype(BF16)
                if k:
                    q3(c, h, k).start()
        with jax.named_scope("rs_fin"):
            for h in range(2):
                rows = pl.ds(h * SUB, SUB)
                total = xg[c, z, y, rows, :].astype(F32) + mid[h, 0].astype(F32)
                for k in (1, 2, 3):
                    q3(c, h, k).wait_recv()
                    total += r4[c, h, k - 1].astype(F32)
                ybuf[c, rows, :] = total.astype(BF16)

        @pl.when(stage < last)
        def _():
            hop_copy(c).start()

        out_copy(c).start()

        for h in range(2):
            for k in range(R):
                if k:
                    p1(c, h, k).wait_send()
                    q3(c, h, k).wait_send()
                for side in range(2):
                    p2(c, h, side, k).wait_send()
                    q2(c, h, side, k).wait_send()
                p3(c, h, k).wait_send()
                q1(c, h, k).wait_send()
        return carry

    lax.fori_loop(0, CHUNKS, chunk, 0)

    for c in range(CHUNKS):
        out_copy(c).wait()

        @pl.when(stage < last)
        def _():
            hop_copy(c).wait_send()


def solution(mesh):
    pp_size = mesh.shape["pp"]
    cos_tab, sin_tab = rope_tables()
    any_spec = pl.BlockSpec(memory_space=pl.ANY)
    vmem_spec = pl.BlockSpec(memory_space=pltpu.VMEM)
    dma = pltpu.SemaphoreType.DMA

    def body(x_in, ln_params, w_q, w_k, w_v, w_o, w_up, w_down):
        flat = HEADS * HD
        wq = jnp.transpose(w_q[0], (1, 2, 3, 0)).reshape(flat, D)
        wk = jnp.transpose(w_k[0], (1, 2, 0)).reshape(flat, D)
        wv = jnp.transpose(w_v[0], (1, 2, 0)).reshape(flat, D)
        wo = w_o[0].reshape(flat, D)
        out = pl.pallas_call(
            functools.partial(kernel, pp_size),
            out_shape=jax.ShapeDtypeStruct(x_in.shape, BF16),
            in_specs=[any_spec, vmem_spec] + [any_spec] * 6 + [vmem_spec, vmem_spec],
            out_specs=any_spec,
            scratch_shapes=[
                pltpu.VMEM((CHUNKS, R, R, BLK, D), BF16),
                pltpu.VMEM((QKV, D), BF16),
                pltpu.VMEM((D, FF), BF16),
                pltpu.VMEM((ACT, D), BF16),
                pltpu.VMEM((2 * GROUP, D), BF16),
                pltpu.VMEM((2 * GROUP, D), BF16),
                pltpu.VMEM((2 * flat, SEQ), BF16),
                pltpu.VMEM((HEADS, SEQ, HD), BF16),
                pltpu.VMEM((SEQ, ACT), BF16),
                pltpu.VMEM((R, R, BLK, D), BF16),
                pltpu.VMEM((CHUNKS, 2, R, SUB, D), BF16),
                pltpu.VMEM((CHUNKS, 2, R, SUB, D), BF16),
                pltpu.VMEM((CHUNKS, 2, R, SUB, D), BF16),
                pltpu.VMEM((2, R, SUB, D), BF16),
                pltpu.VMEM((CHUNKS, 2, R - 1, SUB, D), BF16),
                pltpu.VMEM((CHUNKS, BLK, D), BF16),
                dma((6,)), dma((CHUNKS,)), dma((CHUNKS,)), dma((CHUNKS,)), dma((CHUNKS,)),
                dma((2, 3)), dma((CHUNKS, 2, 3)), dma((2, 2, R)), dma((CHUNKS, 2, 2, R)), dma((2, R)), dma((CHUNKS, 2, R)),
                dma((2, R)), dma((CHUNKS, 2, R)), dma((2, 2, R)), dma((CHUNKS, 2, 2, R)), dma((2, 3)), dma((CHUNKS, 2, 3)),
                pltpu.SemaphoreType.REGULAR,
            ],
            compiler_params=pltpu.CompilerParams(collective_id=1, has_side_effects=True, vmem_limit_bytes=62 * 2**20),
            name="pipeline",
        )(x_in, ln_params[0], wq, wk, wv, wo, w_up[0], w_down[0], jnp.asarray(cos_tab), jnp.asarray(sin_tab))
        return out[None]

    in_specs = (P(None, "dp", "tp", None), P("pp", None, None), P("pp", None, "tp", None, None), P("pp", None, "tp", None), P("pp", None, "tp", None), P("pp", "tp", None, None, None), P("pp", None, "tp"), P("pp", "tp", None))
    return jax.shard_map(body, mesh=mesh, in_specs=in_specs, out_specs=P("pp", None, "dp", "tp", None), check_vma=False)
```

```python
import functools

import jax
import jax.numpy as jnp
import numpy as np
from jax import lax
from jax.experimental import pallas as pl
from jax.experimental.pallas import tpu as pltpu
from jax.sharding import PartitionSpec as P

MESH = pl.DeviceIdType.MESH
LN_EPS = 1e-5
ROPE_BASE = 10000.0
F32, BF16 = jnp.float32, jnp.bfloat16

R = 4
BLK = 32
SEQ = R * R * BLK
D = 2560
SUB = BLK // 2
GROUP = R * BLK
ORDER = (0, 1, 3, 2)
SIDE = (0, 1, 1, 0)
HEADS = 2
HD = 80
HH = HD // 2
FF = 640
QKV = 3 * HEADS * HD
ACT = FF + HEADS * HD
CHUNKS = 4


def rope_tables():
    positions = np.arange(SEQ, dtype=np.float32)
    inv_freq = (np.float32(ROPE_BASE) ** (np.float32(-2.0) * np.arange(HH, dtype=np.float32) / np.float32(HD))).astype(np.float32)
    angles = (inv_freq[:, None] * positions[None, :]).astype(np.float32)
    return np.cos(angles).astype(np.float32), np.sin(angles).astype(np.float32)


def nt_dot(a, b):
    return lax.dot_general(a, b, (((1,), (1,)), ((), ())), preferred_element_type=F32)


def nn_dot(a, b):
    return lax.dot_general(a, b, (((1,), (0,)), ((), ())), preferred_element_type=F32)


def kernel(pp_size, x_ref, ln_ref, wq_ref, wk_ref, wv_ref, wo_ref, wup_ref, wdown_ref, cos_ref, sin_ref, out_ref,
           xg, wqkv, wup, wcat, ha, hm, qv, ks, act, part, r1, r2, r3, mid, r4, ybuf,
           w_sem, in_sem, out_sem, hop_send, hop_recv, p1_send, p1_recv, p2_send, p2_recv, p3_send, p3_recv,
           q1_send, q1_recv, q2_send, q2_recv, q3_send, q3_recv, direct_send, turn_sem):
    tp = lax.axis_index("tp")
    stage = lax.axis_index("pp")
    z, y = lax.div(tp, R), lax.rem(tp, R)
    last = pp_size - 1
    even = lax.rem(stage, 2) == 0
    partner = stage + 1 - 2 * lax.rem(stage, 2)
    nqk = HEADS * HD

    home = ((z, y), (y, z))

    def at(h, v, u):
        return (v, u) if h == 0 else (u, v)

    def peer(h, dv, du, pp=stage):
        v, u = home[h]
        zz, yy = at(h, lax.rem(v + dv, R), lax.rem(u + du, R))
        return {"tp": zz * R + yy, "pp": pp}

    def remote(src, dst, send, recv, device):
        return pltpu.make_async_remote_copy(src_ref=src, dst_ref=dst, send_sem=send, recv_sem=recv, device_id=device, device_id_type=MESH)

    barrier = pltpu.get_barrier_semaphore()
    for d in (1, 2, 3):
        for h in range(2):
            pl.semaphore_signal(barrier, inc=1, device_id=peer(h, 0, d), device_id_type=MESH)
            pl.semaphore_signal(barrier, inc=1, device_id=peer(h, 0, d, partner), device_id_type=MESH)

    @pl.when(stage > 0)
    def _():
        pl.semaphore_signal(barrier, inc=1, device_id={"pp": stage - 1}, device_id_type=MESH)

    @pl.when(stage < last)
    def _():
        pl.semaphore_signal(barrier, inc=1, device_id={"pp": stage + 1}, device_id_type=MESH)

    weight_copies = [
        pltpu.make_async_copy(wq_ref, wqkv.at[pl.ds(0, nqk)], w_sem.at[0]),
        pltpu.make_async_copy(wk_ref, wqkv.at[pl.ds(nqk, nqk)], w_sem.at[1]),
        pltpu.make_async_copy(wv_ref, wqkv.at[pl.ds(2 * nqk, nqk)], w_sem.at[2]),
        pltpu.make_async_copy(wup_ref, wup, w_sem.at[3]),
        pltpu.make_async_copy(wdown_ref, wcat.at[pl.ds(0, FF)], w_sem.at[4]),
        pltpu.make_async_copy(wo_ref, wcat.at[pl.ds(FF, nqk)], w_sem.at[5]),
    ]

    def input_copy(c):
        return pltpu.make_async_copy(x_ref.at[lax.div(c, 2), lax.rem(c, 2)], xg.at[c, z, y], in_sem.at[c])

    @pl.when(stage == 0)
    def _():
        for c in range(CHUNKS):
            input_copy(c).start()

    for cp in weight_copies:
        cp.start()

    pl.semaphore_wait(barrier, 12 + jnp.where(stage > 0, 1, 0) + jnp.where(stage < last, 1, 0))

    def hop_copy(c):
        return remote(ybuf.at[c], xg.at[c, z, y], hop_send.at[c], hop_recv.at[c], {"pp": lax.rem(stage + 1, pp_size)})

    def out_copy(c):
        return pltpu.make_async_copy(ybuf.at[c], out_ref.at[lax.div(c, 2), lax.rem(c, 2)], out_sem.at[c])

    def place(h, dv, du):
        v, u = home[h]
        return at(h, lax.rem(v + dv + R, R), lax.rem(u + du + R, R))

    def gathered(c, h, dv, du):
        zz, yy = place(h, dv, du)
        return xg.at[c, zz, yy, pl.ds(h * SUB, SUB), :]

    def partial_at(h, dv, du):
        zz, yy = place(h, dv, du)
        return part.at[zz, yy, pl.ds(h * SUB, SUB), :]

    def p1(c, h, d, incoming=False):
        view = gathered(c, h, 0, -d if incoming else 0)
        return remote(view, view, p1_send.at[h, d - 1], p1_recv.at[c, h, d - 1], peer(h, 0, d))

    def p2(c, h, side, k, incoming=False):
        view = gathered(c, h, ((-1, 1)[side] if incoming else 0), -k)
        return remote(view, view, p2_send.at[h, side, k], p2_recv.at[c, h, side, k], peer(h, (1, R - 1)[side], 0))

    def p3(c, h, k, incoming=False):
        side = SIDE[k]
        view = gathered(c, h, 2 if incoming else (-1, 1)[side] if k else 0, -k)
        return remote(view, view, p3_send.at[h, k], p3_recv.at[c, h, k], peer(h, (1, R - 1)[side] if k else 2, 0))

    def q1(c, h, k):
        return remote(partial_at(h, 2, -k), r1.at[c, h, k], q1_send.at[h, k], q1_recv.at[c, h, k], peer(h, (1, R - 1)[SIDE[k]] if k else 2, 0))

    def q2(c, h, side, k):
        return remote(partial_at(h, (1, -1)[side], -k), (r2 if side == 0 else r3).at[c, h, k], q2_send.at[h, side, k], q2_recv.at[c, h, side, k],
                      peer(h, (1, R - 1)[side], 0))

    def q3(c, h, k):
        return remote(mid.at[h, k], r4.at[c, h, k - 1], q3_send.at[h, k - 1], q3_recv.at[c, h, k - 1], peer(h, 0, R - k))

    def first_sends(c, direct=False):
        src_dev = stage + 1 if direct else stage
        copies = []
        for h in range(2):
            for i, (hh, dv, du) in enumerate([(h, 0, 1), (h, 0, 3), (1 - h, 1, 0), (1 - h, 3, 0), (h, 0, 2), (1 - h, 2, 0)]):
                dst = gathered(c, hh, 0, 0)
                src = ybuf.at[c, pl.ds(hh * SUB, SUB), :] if direct else dst
                if du:
                    send, recv = p1_send.at[hh, du - 1], p1_recv.at[c, hh, du - 1]
                elif dv == 2:
                    send, recv = p3_send.at[hh, 0], p3_recv.at[c, hh, 0]
                else:
                    send, recv = p2_send.at[hh, dv // 2, 0], p2_recv.at[c, hh, dv // 2, 0]
                copies.append(remote(src, dst, direct_send.at[c, h, i] if direct else send, recv, peer(hh, dv, du, src_dev)))
        return copies

    def norms(c, blocks):
        for h, dv, du in blocks:
            block = gathered(c, h, dv, du)
            zz, yy = place(h, dv, du)
            total = jnp.sum(block[...].astype(F32), axis=-1, keepdims=True)
            mean = total * (1.0 / D)
            dev = block[...].astype(F32) - mean
            var = jnp.sum(dev * dev, axis=-1, keepdims=True) * (1.0 / D)
            scale = lax.rsqrt(var + LN_EPS)
            unit = (block[...].astype(F32) - mean) * scale
            dst = pl.ds(pl.multiple_of(zz * GROUP + yy * BLK + h * SUB, SUB), SUB)
            ha[dst, :] = (unit * ln_ref[0:1, :] + ln_ref[1:2, :]).astype(BF16)
            hm[dst, :] = (unit * ln_ref[2:3, :] + ln_ref[3:4, :]).astype(BF16)

    def project(offs):
        toks = [pl.ds(pl.multiple_of(lax.rem(z + off, R) * GROUP, GROUP), GROUP) for off in offs]

        proj = nt_dot(wqkv[...], jnp.concatenate([ha[tok, :] for tok in toks], axis=0))
        for slot, tok in enumerate(toks):
            cols = proj[:, slot * GROUP:(slot + 1) * GROUP]
            cos, sin = cos_ref[:, tok], sin_ref[:, tok]

            def rope(row):
                first, second = cols[row:row + HH], cols[row + HH:row + HD]
                return jnp.concatenate([first * cos - second * sin, second * cos + first * sin], axis=0)

            for hd in range(HEADS):
                qv[pl.ds(hd * HD, HD), tok] = rope(hd * HD).astype(BF16)
                ks[hd, tok, :] = rope(nqk + hd * HD).T.astype(BF16)
            qv[pl.ds(nqk, nqk), tok] = cols[2 * nqk:].astype(BF16)

        for tok in toks:
            pre = nn_dot(hm[tok, :], wup[...])
            act[tok, 0:FF] = (0.5 * pre * (1.0 + lax.erf(pre * np.float32(0.5 ** 0.5)))).astype(BF16)

    def chunk(c, carry):
        with jax.named_scope("wait_in"):
            @pl.when(stage == 0)
            def _():
                input_copy(c).wait()

            @pl.when(stage > 0)
            def _():
                hop_copy(c).wait_recv()

            @pl.when((c > 0) & even)
            def _():
                pl.semaphore_wait(turn_sem, 1)

            @pl.when(even)
            def _():
                for cp in first_sends(c):
                    cp.start()

        with jax.named_scope("p1_wait"):
            for k in ORDER[1:]:
                for h in range(2):
                    p1(c, h, k, True).wait_recv()
                    for side in range(2):
                        p2(c, h, side, k).start()
        with jax.named_scope("norm_a"):
            norms(c, [(h, 0, -k) for k in ORDER for h in range(2)])
        with jax.named_scope("wait_b"):
            for h in (1, 0):
                for side in range(2):
                    p2(c, h, side, 0, True).wait_recv()
                p3(c, h, 0, True).wait_recv()
        with jax.named_scope("norm_b"):
            norms(c, [(h, dv, 0) for h in (1, 0) for dv in (-1, 1, 2)])
        def rest(k):
            for h in range(2):
                p2(c, h, 1 - SIDE[k], k, True).wait_recv()
            norms(c, [(h, dv, -k) for h in range(2) for dv in (-1, 1)])

        with jax.named_scope("forward"):
            for k in ORDER[1:]:
                for h in range(2):
                    p2(c, h, SIDE[k], k, True).wait_recv()
                    p3(c, h, k).start()
                if k != ORDER[-1]:
                    rest(k)

        @pl.when((c < CHUNKS - 1) & jnp.logical_not(even))
        def _():
            pl.semaphore_signal(turn_sem, inc=1, device_id={"pp": stage - 1}, device_id_type=MESH)

        @pl.when(c == 0)
        def _():
            for cp in weight_copies:
                cp.wait()

        with jax.named_scope("proj0"):
            project((0,))
        with jax.named_scope("norm_c"):
            rest(ORDER[-1])
        with jax.named_scope("wait_e"):
            for k in (1, 3):
                p3(c, 1, k, True).wait_recv()
        with jax.named_scope("norm_e"):
            norms(c, [(1, 2, -1), (1, 2, -3)])
        with jax.named_scope("proj31"):
            project((3, 1))
        with jax.named_scope("wait_f"):
            p3(c, 1, 2, True).wait_recv()
            for k in ORDER[1:]:
                p3(c, 0, k, True).wait_recv()
        with jax.named_scope("norm_f"):
            norms(c, [(1, 2, -2)] + [(0, 2, -k) for k in ORDER[1:]])
        with jax.named_scope("proj2"):
            project((2,))

        with jax.named_scope("attn"):
            for qb in range(2):
                toks = pl.ds(qb * 256, 256)
                nk = (qb + 1) * 256
                ctx = []
                for hd in range(HEADS):
                    scores = nn_dot(ks[hd, 0:nk, :], qv[pl.ds(hd * HD, HD), toks]) * (HD ** -0.5)
                    key_pos = lax.broadcasted_iota(jnp.int32, (nk, 256), 0)
                    query_pos = lax.broadcasted_iota(jnp.int32, (nk, 256), 1) + qb * 256
                    scores = jnp.where(query_pos >= key_pos, scores, -1e30)
                    top = jnp.max(scores, axis=0, keepdims=True)
                    probs = jnp.exp(scores - top)
                    total = jnp.sum(probs, axis=0, keepdims=True)
                    probs = (probs * (1.0 / total)).astype(BF16)
                    ctx.append(nn_dot(qv[pl.ds(nqk + hd * HD, HD), 0:nk], probs))
                act[toks, FF:ACT] = jnp.concatenate(ctx, axis=0).T.astype(BF16)

        def down(blocks):
            rows = []
            for h, dv, du in blocks:
                zz, yy = place(h, dv, du)
                rows.append(act[pl.ds(pl.multiple_of(zz * GROUP + yy * BLK + h * SUB, SUB), SUB), :])
            out = nn_dot(jnp.concatenate(rows, axis=0), wcat[...]).astype(BF16)
            for i, (h, dv, du) in enumerate(blocks):
                partial_at(h, dv, du)[...] = out[i * SUB:(i + 1) * SUB]

        with jax.named_scope("down"):
            down([(h, 2, -k) for h in range(2) for k in ORDER])
            for k in (1, 3, 2, 0):
                for h in range(2):
                    q1(c, h, k).start()
            for h in range(2):
                down([(h, dv, -k) for dv in (1, -1) for k in ORDER])
                for k in ORDER:
                    for side in range(2):
                        if k == 0 or SIDE[k] != side:
                            q2(c, h, side, k).start()
            down([(h, 0, -k) for h in range(2) for k in ORDER])

        with jax.named_scope("rs_add"):
            for h, k in [(0, 1), (1, 1), (0, 3), (1, 3), (0, 2), (1, 2)]:
                side = SIDE[k]
                q1(c, h, k).wait_recv()
                mine = partial_at(h, (1, -1)[side], -k)
                mine[...] = (mine[...].astype(F32) + r1[c, h, k].astype(F32)).astype(BF16)
                q2(c, h, side, k).start()
        with jax.named_scope("rs_mid"):
            for h, k in [(0, 1), (1, 1), (0, 3), (1, 3), (0, 2), (1, 2), (0, 0), (1, 0)]:
                q2(c, h, 0, k).wait_recv()
                q2(c, h, 1, k).wait_recv()
                total = partial_at(h, 0, -k)[...].astype(F32) + r2[c, h, k].astype(F32) + r3[c, h, k].astype(F32)
                if k == 0:
                    q1(c, h, 0).wait_recv()
                    total += r1[c, h, 0].astype(F32)
                mid[h, k] = total.astype(BF16)
                if k:
                    q3(c, h, k).start()
        with jax.named_scope("rs_fin"):
            for h in range(2):
                rows = pl.ds(h * SUB, SUB)
                total = xg[c, z, y, rows, :].astype(F32) + mid[h, 0].astype(F32)
                for k in (1, 2, 3):
                    q3(c, h, k).wait_recv()
                    total += r4[c, h, k - 1].astype(F32)
                ybuf[c, rows, :] = total.astype(BF16)

        @pl.when(stage < last)
        def _():
            hop_copy(c).start()

        @pl.when(even)
        def _():
            for cp in first_sends(c, True):
                cp.start()

        out_copy(c).start()

        @pl.when(even)
        def _():
            for cp in first_sends(c):
                cp.wait_send()

        for h in range(2):
            for k in range(R):
                if k:
                    q3(c, h, k).wait_send()
                    p3(c, h, k).wait_send()
                for side in range(2):
                    if k:
                        p2(c, h, side, k).wait_send()
                    q2(c, h, side, k).wait_send()
                q1(c, h, k).wait_send()
        return carry

    lax.fori_loop(0, CHUNKS, chunk, 0)

    for c in range(CHUNKS):
        out_copy(c).wait()

        @pl.when(stage < last)
        def _():
            hop_copy(c).wait_send()

        @pl.when(even)
        def _():
            for cp in first_sends(c, True):
                cp.wait_send()


def solution(mesh):
    pp_size = mesh.shape["pp"]
    cos_tab, sin_tab = rope_tables()
    any_spec = pl.BlockSpec(memory_space=pl.ANY)
    vmem_spec = pl.BlockSpec(memory_space=pltpu.VMEM)
    dma = pltpu.SemaphoreType.DMA

    def body(x_in, ln_params, w_q, w_k, w_v, w_o, w_up, w_down):
        flat = HEADS * HD
        wq = jnp.transpose(w_q[0], (1, 2, 3, 0)).reshape(flat, D)
        wk = jnp.transpose(w_k[0], (1, 2, 0)).reshape(flat, D)
        wv = jnp.transpose(w_v[0], (1, 2, 0)).reshape(flat, D)
        wo = w_o[0].reshape(flat, D)
        out = pl.pallas_call(
            functools.partial(kernel, pp_size),
            out_shape=jax.ShapeDtypeStruct(x_in.shape, BF16),
            in_specs=[any_spec, vmem_spec] + [any_spec] * 6 + [vmem_spec, vmem_spec],
            out_specs=any_spec,
            scratch_shapes=[
                pltpu.VMEM((CHUNKS, R, R, BLK, D), BF16),
                pltpu.VMEM((QKV, D), BF16),
                pltpu.VMEM((D, FF), BF16),
                pltpu.VMEM((ACT, D), BF16),
                pltpu.VMEM((SEQ, D), BF16),
                pltpu.VMEM((SEQ, D), BF16),
                pltpu.VMEM((2 * flat, SEQ), BF16),
                pltpu.VMEM((HEADS, SEQ, HD), BF16),
                pltpu.VMEM((SEQ, ACT), BF16),
                pltpu.VMEM((R, R, BLK, D), BF16),
                pltpu.VMEM((CHUNKS, 2, R, SUB, D), BF16),
                pltpu.VMEM((CHUNKS, 2, R, SUB, D), BF16),
                pltpu.VMEM((CHUNKS, 2, R, SUB, D), BF16),
                pltpu.VMEM((2, R, SUB, D), BF16),
                pltpu.VMEM((CHUNKS, 2, R - 1, SUB, D), BF16),
                pltpu.VMEM((CHUNKS, BLK, D), BF16),
                dma((6,)), dma((CHUNKS,)), dma((CHUNKS,)), dma((CHUNKS,)), dma((CHUNKS,)),
                dma((2, 3)), dma((CHUNKS, 2, 3)), dma((2, 2, R)), dma((CHUNKS, 2, 2, R)), dma((2, R)), dma((CHUNKS, 2, R)),
                dma((2, R)), dma((CHUNKS, 2, R)), dma((2, 2, R)), dma((CHUNKS, 2, 2, R)), dma((2, 3)), dma((CHUNKS, 2, 3)),
                dma((CHUNKS, 2, 6)), pltpu.SemaphoreType.REGULAR,
            ],
            compiler_params=pltpu.CompilerParams(collective_id=1, has_side_effects=True, vmem_limit_bytes=62 * 2**20),
            name="pipeline",
        )(x_in, ln_params[0], wq, wk, wv, wo, w_up[0], w_down[0], jnp.asarray(cos_tab), jnp.asarray(sin_tab))
        return out[None]

    in_specs = (P(None, "dp", "tp", None), P("pp", None, None), P("pp", None, "tp", None, None), P("pp", None, "tp", None), P("pp", None, "tp", None), P("pp", "tp", None, None, None), P("pp", None, "tp"), P("pp", "tp", None))
    return jax.shard_map(body, mesh=mesh, in_specs=in_specs, out_specs=P("pp", None, "dp", "tp", None), check_vma=False)
```

```python
import functools

import jax
import jax.numpy as jnp
import numpy as np
from jax import lax
from jax.experimental import pallas as pl
from jax.experimental.pallas import tpu as pltpu
from jax.sharding import PartitionSpec as P

MESH = pl.DeviceIdType.MESH
LN_EPS = 1e-5
ROPE_BASE = 10000.0
F32, BF16 = jnp.float32, jnp.bfloat16

R = 4
BLK = 32
SEQ = R * R * BLK
D = 2560
SUB = BLK // 2
GROUP = R * BLK
ORDER = (0, 1, 3, 2)
LATE = ((0, 1), (0, 3), (1, 3), (0, 2), (1, 2))
SIDE = (0, 1, 1, 0)
HEADS = 2
HD = 80
HH = HD // 2
FF = 640
QKV = 3 * HEADS * HD
ACT = FF + HEADS * HD
CHUNKS = 4


def rope_tables():
    positions = np.arange(SEQ, dtype=np.float32)
    inv_freq = (np.float32(ROPE_BASE) ** (np.float32(-2.0) * np.arange(HH, dtype=np.float32) / np.float32(HD))).astype(np.float32)
    angles = (inv_freq[:, None] * positions[None, :]).astype(np.float32)
    return np.cos(angles).astype(np.float32), np.sin(angles).astype(np.float32)


def nt_dot(a, b):
    return lax.dot_general(a, b, (((1,), (1,)), ((), ())), preferred_element_type=F32)


def nn_dot(a, b):
    return lax.dot_general(a, b, (((1,), (0,)), ((), ())), preferred_element_type=F32)


def kernel(pp_size, x_ref, ln_ref, wq_ref, wk_ref, wv_ref, wo_ref, wup_ref, wdown_ref, cos_ref, sin_ref, out_ref,
           xg, wqkv, wup, wcat, ha, hm, qv, ks, act, part, r1, r2, r3, mid, r4, ybuf,
           w_sem, in_sem, out_sem, hop_send, hop_recv, p1_send, p1_recv, p2_send, p2_recv, p3_send, p3_recv,
           q1_send, q1_recv, q2_send, q2_recv, q3_send, q3_recv, direct_send, turn_sem):
    tp = lax.axis_index("tp")
    stage = lax.axis_index("pp")
    z, y = lax.div(tp, R), lax.rem(tp, R)
    last = pp_size - 1
    even = lax.rem(stage, 2) == 0
    partner = stage + 1 - 2 * lax.rem(stage, 2)
    nqk = HEADS * HD

    home = ((z, y), (y, z))

    def at(h, v, u):
        return (v, u) if h == 0 else (u, v)

    def peer(h, dv, du, pp=stage):
        v, u = home[h]
        zz, yy = at(h, lax.rem(v + dv, R), lax.rem(u + du, R))
        return {"tp": zz * R + yy, "pp": pp}

    def remote(src, dst, send, recv, device):
        return pltpu.make_async_remote_copy(src_ref=src, dst_ref=dst, send_sem=send, recv_sem=recv, device_id=device, device_id_type=MESH)

    barrier = pltpu.get_barrier_semaphore()
    for d in (1, 2, 3):
        for h in range(2):
            pl.semaphore_signal(barrier, inc=1, device_id=peer(h, 0, d), device_id_type=MESH)
            pl.semaphore_signal(barrier, inc=1, device_id=peer(h, 0, d, partner), device_id_type=MESH)

    @pl.when(stage > 0)
    def _():
        pl.semaphore_signal(barrier, inc=1, device_id={"pp": stage - 1}, device_id_type=MESH)

    @pl.when(stage < last)
    def _():
        pl.semaphore_signal(barrier, inc=1, device_id={"pp": stage + 1}, device_id_type=MESH)

    weight_copies = [
        pltpu.make_async_copy(wq_ref, wqkv.at[pl.ds(0, nqk)], w_sem.at[0]),
        pltpu.make_async_copy(wk_ref, wqkv.at[pl.ds(nqk, nqk)], w_sem.at[1]),
        pltpu.make_async_copy(wv_ref, wqkv.at[pl.ds(2 * nqk, nqk)], w_sem.at[2]),
        pltpu.make_async_copy(wup_ref, wup, w_sem.at[3]),
        pltpu.make_async_copy(wdown_ref, wcat.at[pl.ds(0, FF)], w_sem.at[4]),
        pltpu.make_async_copy(wo_ref, wcat.at[pl.ds(FF, nqk)], w_sem.at[5]),
    ]

    def input_copy(c):
        return pltpu.make_async_copy(x_ref.at[lax.div(c, 2), lax.rem(c, 2)], xg.at[c, z, y], in_sem.at[c])

    @pl.when(stage == 0)
    def _():
        for c in range(CHUNKS):
            input_copy(c).start()

    for cp in weight_copies:
        cp.start()

    pl.semaphore_wait(barrier, 12 + jnp.where(stage > 0, 1, 0) + jnp.where(stage < last, 1, 0))

    def hop_copy(c):
        return remote(ybuf.at[c], xg.at[c, z, y], hop_send.at[c], hop_recv.at[c], {"pp": lax.rem(stage + 1, pp_size)})

    def out_copy(c):
        return pltpu.make_async_copy(ybuf.at[c], out_ref.at[lax.div(c, 2), lax.rem(c, 2)], out_sem.at[c])

    def place(h, dv, du):
        v, u = home[h]
        return at(h, lax.rem(v + dv + R, R), lax.rem(u + du + R, R))

    def gathered(c, h, dv, du):
        zz, yy = place(h, dv, du)
        return xg.at[c, zz, yy, pl.ds(h * SUB, SUB), :]

    def partial_at(h, dv, du):
        zz, yy = place(h, dv, du)
        return part.at[zz, yy, pl.ds(h * SUB, SUB), :]

    def p1(c, h, d, incoming=False):
        view = gathered(c, h, 0, -d if incoming else 0)
        return remote(view, view, p1_send.at[h, d - 1], p1_recv.at[c, h, d - 1], peer(h, 0, d))

    def p2(c, h, side, k, incoming=False):
        view = gathered(c, h, ((-1, 1)[side] if incoming else 0), -k)
        return remote(view, view, p2_send.at[h, side, k], p2_recv.at[c, h, side, k], peer(h, (1, R - 1)[side], 0))

    def p3(c, h, k, incoming=False):
        side = SIDE[k]
        view = gathered(c, h, 2 if incoming else (-1, 1)[side] if k else 0, -k)
        return remote(view, view, p3_send.at[h, k], p3_recv.at[c, h, k], peer(h, (1, R - 1)[side] if k else 2, 0))

    def q1(c, h, k):
        return remote(partial_at(h, 2, -k), r1.at[c, h, k], q1_send.at[h, k], q1_recv.at[c, h, k], peer(h, (1, R - 1)[SIDE[k]], 0))

    def q2(c, h, side, k):
        return remote(partial_at(h, (1, -1)[side], -k), (r2 if side == 0 else r3).at[c, h, k], q2_send.at[h, side, k], q2_recv.at[c, h, side, k],
                      peer(h, (1, R - 1)[side], 0))

    def q3(c, h, k):
        return remote(mid.at[h, k], r4.at[c, h, k - 1], q3_send.at[h, k - 1], q3_recv.at[c, h, k - 1], peer(h, 0, R - k))

    def first_sends(c, direct=False):
        src_dev = stage + 1 if direct else stage
        copies = []
        for h in range(2):
            for i, (hh, dv, du) in enumerate([(h, 0, 1), (h, 0, 3), (1 - h, 1, 0), (1 - h, 3, 0), (h, 0, 2), (1 - h, 2, 0)]):
                dst = gathered(c, hh, 0, 0)
                src = ybuf.at[c, pl.ds(hh * SUB, SUB), :] if direct else dst
                if du:
                    send, recv = p1_send.at[hh, du - 1], p1_recv.at[c, hh, du - 1]
                elif dv == 2:
                    send, recv = p3_send.at[hh, 0], p3_recv.at[c, hh, 0]
                else:
                    send, recv = p2_send.at[hh, dv // 2, 0], p2_recv.at[c, hh, dv // 2, 0]
                copies.append(remote(src, dst, direct_send.at[c, h, i] if direct else send, recv, peer(hh, dv, du, src_dev)))
        return copies

    def norms(c, blocks):
        for h, dv, du in blocks:
            block = gathered(c, h, dv, du)
            zz, yy = place(h, dv, du)
            total = jnp.sum(block[...].astype(F32), axis=-1, keepdims=True)
            mean = total * (1.0 / D)
            dev = block[...].astype(F32) - mean
            var = jnp.sum(dev * dev, axis=-1, keepdims=True) * (1.0 / D)
            scale = lax.rsqrt(var + LN_EPS)
            unit = (block[...].astype(F32) - mean) * scale
            dst = pl.ds(pl.multiple_of(zz * GROUP + yy * BLK + h * SUB, SUB), SUB)
            ha[dst, :] = (unit * ln_ref[0:1, :] + ln_ref[1:2, :]).astype(BF16)
            hm[dst, :] = (unit * ln_ref[2:3, :] + ln_ref[3:4, :]).astype(BF16)

    def project(offs):
        toks = [pl.ds(pl.multiple_of(lax.rem(z + off, R) * GROUP, GROUP), GROUP) for off in offs]

        proj = nt_dot(wqkv[...], jnp.concatenate([ha[tok, :] for tok in toks], axis=0))
        for slot, tok in enumerate(toks):
            cols = proj[:, slot * GROUP:(slot + 1) * GROUP]
            cos, sin = cos_ref[:, tok], sin_ref[:, tok]

            def rope(row):
                first, second = cols[row:row + HH], cols[row + HH:row + HD]
                return jnp.concatenate([first * cos - second * sin, second * cos + first * sin], axis=0)

            for hd in range(HEADS):
                qv[pl.ds(hd * HD, HD), tok] = rope(hd * HD).astype(BF16)
                ks[hd, tok, :] = rope(nqk + hd * HD).T.astype(BF16)
            qv[pl.ds(nqk, nqk), tok] = cols[2 * nqk:].astype(BF16)

        for tok in toks:
            pre = nn_dot(hm[tok, :], wup[...])
            act[tok, 0:FF] = (0.5 * pre * (1.0 + lax.erf(pre * np.float32(0.5 ** 0.5)))).astype(BF16)

    def chunk(c, carry):
        with jax.named_scope("wait_in"):
            @pl.when(stage == 0)
            def _():
                input_copy(c).wait()

            @pl.when(stage > 0)
            def _():
                hop_copy(c).wait_recv()

            @pl.when((c > 0) & even)
            def _():
                pl.semaphore_wait(turn_sem, 1)

            @pl.when(even)
            def _():
                for cp in first_sends(c):
                    cp.start()

        with jax.named_scope("p1_wait"):
            for k in ORDER[1:]:
                for h in range(2):
                    p1(c, h, k, True).wait_recv()
                    for side in range(2):
                        p2(c, h, side, k).start()
        with jax.named_scope("norm_a"):
            norms(c, [(h, 0, -k) for k in ORDER for h in range(2)])
        with jax.named_scope("wait_b"):
            for h in (1, 0):
                for side in range(2):
                    p2(c, h, side, 0, True).wait_recv()
                p3(c, h, 0, True).wait_recv()
        with jax.named_scope("norm_b"):
            norms(c, [(h, dv, 0) for h in (1, 0) for dv in (-1, 1, 2)])
        def rest(k):
            for h in range(2):
                p2(c, h, 1 - SIDE[k], k, True).wait_recv()
            norms(c, [(h, dv, -k) for h in range(2) for dv in (-1, 1)])

        with jax.named_scope("forward"):
            for k in ORDER[1:]:
                for h in range(2):
                    p2(c, h, SIDE[k], k, True).wait_recv()
                    p3(c, h, k).start()
                if k != ORDER[-1]:
                    rest(k)

        @pl.when((c < CHUNKS - 1) & jnp.logical_not(even))
        def _():
            pl.semaphore_signal(turn_sem, inc=1, device_id={"pp": stage - 1}, device_id_type=MESH)

        @pl.when(c == 0)
        def _():
            for cp in weight_copies:
                cp.wait()

        with jax.named_scope("norm_c"):
            rest(ORDER[-1])
        with jax.named_scope("wait_e"):
            p3(c, 1, 1, True).wait_recv()
        with jax.named_scope("norm_e"):
            norms(c, [(1, 2, -1)])
        with jax.named_scope("proj03"):
            project((0, 3))
        with jax.named_scope("wait_f"):
            for h, k in LATE:
                p3(c, h, k, True).wait_recv()
        with jax.named_scope("norm_f"):
            norms(c, [(h, 2, -k) for h, k in LATE])
        with jax.named_scope("proj12"):
            project((1, 2))

        with jax.named_scope("attn"):
            for qb in range(2):
                toks = pl.ds(qb * 256, 256)
                nk = (qb + 1) * 256
                ctx = []
                for hd in range(HEADS):
                    scores = nn_dot(ks[hd, 0:nk, :], qv[pl.ds(hd * HD, HD), toks]) * (HD ** -0.5)
                    key_pos = lax.broadcasted_iota(jnp.int32, (nk, 256), 0)
                    query_pos = lax.broadcasted_iota(jnp.int32, (nk, 256), 1) + qb * 256
                    scores = jnp.where(query_pos >= key_pos, scores, -1e30)
                    top = jnp.max(scores, axis=0, keepdims=True)
                    probs = jnp.exp(scores - top)
                    total = jnp.sum(probs, axis=0, keepdims=True)
                    probs = (probs * (1.0 / total)).astype(BF16)
                    ctx.append(nn_dot(qv[pl.ds(nqk + hd * HD, HD), 0:nk], probs))
                act[toks, FF:ACT] = jnp.concatenate(ctx, axis=0).T.astype(BF16)

        def down(blocks):
            rows = []
            for h, dv, du in blocks:
                zz, yy = place(h, dv, du)
                rows.append(act[pl.ds(pl.multiple_of(zz * GROUP + yy * BLK + h * SUB, SUB), SUB), :])
            out = nn_dot(jnp.concatenate(rows, axis=0), wcat[...]).astype(BF16)
            for i, (h, dv, du) in enumerate(blocks):
                partial_at(h, dv, du)[...] = out[i * SUB:(i + 1) * SUB]

        with jax.named_scope("down"):
            down([(h, 2, -k) for h in range(2) for k in ORDER])
            for k in (1, 3, 2, 0):
                for h in range(2):
                    q1(c, h, k).start()
            for h in range(2):
                down([(h, dv, -k) for dv in (1, -1) for k in ORDER])
                for k in ORDER:
                    for side in range(2):
                        if SIDE[k] != side:
                            q2(c, h, side, k).start()
            down([(h, 0, -k) for h in range(2) for k in ORDER])

        with jax.named_scope("rs_add"):
            for h, k in [(0, 1), (1, 1), (0, 3), (1, 3), (0, 2), (1, 2), (0, 0), (1, 0)]:
                side = SIDE[k]
                q1(c, h, k).wait_recv()
                mine = partial_at(h, (1, -1)[side], -k)
                mine[...] = (mine[...].astype(F32) + r1[c, h, k].astype(F32)).astype(BF16)
                q2(c, h, side, k).start()
        with jax.named_scope("rs_mid"):
            for h, k in [(0, 1), (1, 1), (0, 3), (1, 3), (0, 2), (1, 2), (0, 0), (1, 0)]:
                q2(c, h, 0, k).wait_recv()
                q2(c, h, 1, k).wait_recv()
                total = partial_at(h, 0, -k)[...].astype(F32) + r2[c, h, k].astype(F32) + r3[c, h, k].astype(F32)
                mid[h, k] = total.astype(BF16)
                if k:
                    q3(c, h, k).start()
        with jax.named_scope("rs_fin"):
            for h in range(2):
                rows = pl.ds(h * SUB, SUB)
                total = xg[c, z, y, rows, :].astype(F32) + mid[h, 0].astype(F32)
                for k in (1, 2, 3):
                    q3(c, h, k).wait_recv()
                    total += r4[c, h, k - 1].astype(F32)
                ybuf[c, rows, :] = total.astype(BF16)

        @pl.when(stage < last)
        def _():
            hop_copy(c).start()

        @pl.when(even)
        def _():
            for cp in first_sends(c, True):
                cp.start()

        out_copy(c).start()

        @pl.when(even)
        def _():
            for cp in first_sends(c):
                cp.wait_send()

        for h in range(2):
            for k in range(R):
                if k:
                    q3(c, h, k).wait_send()
                    p3(c, h, k).wait_send()
                for side in range(2):
                    if k:
                        p2(c, h, side, k).wait_send()
                    q2(c, h, side, k).wait_send()
                q1(c, h, k).wait_send()
        return carry

    lax.fori_loop(0, CHUNKS, chunk, 0)

    for c in range(CHUNKS):
        out_copy(c).wait()

        @pl.when(stage < last)
        def _():
            hop_copy(c).wait_send()

        @pl.when(even)
        def _():
            for cp in first_sends(c, True):
                cp.wait_send()


def solution(mesh):
    pp_size = mesh.shape["pp"]
    cos_tab, sin_tab = rope_tables()
    any_spec = pl.BlockSpec(memory_space=pl.ANY)
    vmem_spec = pl.BlockSpec(memory_space=pltpu.VMEM)
    dma = pltpu.SemaphoreType.DMA

    def body(x_in, ln_params, w_q, w_k, w_v, w_o, w_up, w_down):
        flat = HEADS * HD
        wq = jnp.transpose(w_q[0], (1, 2, 3, 0)).reshape(flat, D)
        wk = jnp.transpose(w_k[0], (1, 2, 0)).reshape(flat, D)
        wv = jnp.transpose(w_v[0], (1, 2, 0)).reshape(flat, D)
        wo = w_o[0].reshape(flat, D)
        out = pl.pallas_call(
            functools.partial(kernel, pp_size),
            out_shape=jax.ShapeDtypeStruct(x_in.shape, BF16),
            in_specs=[any_spec, vmem_spec] + [any_spec] * 6 + [vmem_spec, vmem_spec],
            out_specs=any_spec,
            scratch_shapes=[
                pltpu.VMEM((CHUNKS, R, R, BLK, D), BF16),
                pltpu.VMEM((QKV, D), BF16),
                pltpu.VMEM((D, FF), BF16),
                pltpu.VMEM((ACT, D), BF16),
                pltpu.VMEM((SEQ, D), BF16),
                pltpu.VMEM((SEQ, D), BF16),
                pltpu.VMEM((2 * flat, SEQ), BF16),
                pltpu.VMEM((HEADS, SEQ, HD), BF16),
                pltpu.VMEM((SEQ, ACT), BF16),
                pltpu.VMEM((R, R, BLK, D), BF16),
                pltpu.VMEM((CHUNKS, 2, R, SUB, D), BF16),
                pltpu.VMEM((CHUNKS, 2, R, SUB, D), BF16),
                pltpu.VMEM((CHUNKS, 2, R, SUB, D), BF16),
                pltpu.VMEM((2, R, SUB, D), BF16),
                pltpu.VMEM((CHUNKS, 2, R - 1, SUB, D), BF16),
                pltpu.VMEM((CHUNKS, BLK, D), BF16),
                dma((6,)), dma((CHUNKS,)), dma((CHUNKS,)), dma((CHUNKS,)), dma((CHUNKS,)),
                dma((2, 3)), dma((CHUNKS, 2, 3)), dma((2, 2, R)), dma((CHUNKS, 2, 2, R)), dma((2, R)), dma((CHUNKS, 2, R)),
                dma((2, R)), dma((CHUNKS, 2, R)), dma((2, 2, R)), dma((CHUNKS, 2, 2, R)), dma((2, 3)), dma((CHUNKS, 2, 3)),
                dma((CHUNKS, 2, 6)), pltpu.SemaphoreType.REGULAR,
            ],
            compiler_params=pltpu.CompilerParams(collective_id=1, has_side_effects=True, vmem_limit_bytes=62 * 2**20),
            name="pipeline",
        )(x_in, ln_params[0], wq, wk, wv, wo, w_up[0], w_down[0], jnp.asarray(cos_tab), jnp.asarray(sin_tab))
        return out[None]

    in_specs = (P(None, "dp", "tp", None), P("pp", None, None), P("pp", None, "tp", None, None), P("pp", None, "tp", None), P("pp", None, "tp", None), P("pp", "tp", None, None, None), P("pp", None, "tp"), P("pp", "tp", None))
    return jax.shard_map(body, mesh=mesh, in_specs=in_specs, out_specs=P("pp", None, "dp", "tp", None), check_vma=False)
```

```python
import functools

import jax
import jax.numpy as jnp
import numpy as np
from jax import lax
from jax.experimental import pallas as pl
from jax.experimental.pallas import tpu as pltpu
from jax.sharding import PartitionSpec as P

MESH = pl.DeviceIdType.MESH
LN_EPS = 1e-5
ROPE_BASE = 10000.0
F32, BF16 = jnp.float32, jnp.bfloat16

R = 4
BLK = 32
SEQ = R * R * BLK
D = 2560
SUB = BLK // 2
GROUP = R * BLK
ORDER = (0, 1, 3, 2)
BACK = (2, 1, 3, 0)
LATE = ((0, 1), (0, 3), (1, 3), (0, 2), (1, 2))
SIDE = (0, 1, 1, 0)
HEADS = 2
HD = 80
HH = HD // 2
FF = 640
QKV = 3 * HEADS * HD
ACT = FF + HEADS * HD
CHUNKS = 4


def rope_tables():
    positions = np.arange(SEQ, dtype=np.float32)
    inv_freq = (np.float32(ROPE_BASE) ** (np.float32(-2.0) * np.arange(HH, dtype=np.float32) / np.float32(HD))).astype(np.float32)
    angles = (inv_freq[:, None] * positions[None, :]).astype(np.float32)
    return np.cos(angles).astype(np.float32), np.sin(angles).astype(np.float32)


def nt_dot(a, b):
    return lax.dot_general(a, b, (((1,), (1,)), ((), ())), preferred_element_type=F32)


def nn_dot(a, b):
    return lax.dot_general(a, b, (((1,), (0,)), ((), ())), preferred_element_type=F32)


def kernel(pp_size, x_ref, ln_ref, wq_ref, wk_ref, wv_ref, wo_ref, wup_ref, wdown_ref, cos_ref, sin_ref, out_ref,
           xg, wqkv, wup, wcat, ha, hm, qv, ks, act, part, r1, r2, r3, mid, r4, ybuf,
           w_sem, in_sem, out_sem, hop_send, hop_recv, p1_send, p1_recv, p2_send, p2_recv, p3_send, p3_recv,
           q1_send, q1_recv, q2_send, q2_recv, q3_send, q3_recv, direct_send, turn_sem):
    tp = lax.axis_index("tp")
    stage = lax.axis_index("pp")
    z, y = lax.div(tp, R), lax.rem(tp, R)
    last = pp_size - 1
    even = lax.rem(stage, 2) == 0
    partner = stage + 1 - 2 * lax.rem(stage, 2)
    nqk = HEADS * HD

    home = ((z, y), (y, z))

    def at(h, v, u):
        return (v, u) if h == 0 else (u, v)

    def peer(h, dv, du, pp=stage):
        v, u = home[h]
        zz, yy = at(h, lax.rem(v + dv, R), lax.rem(u + du, R))
        return {"tp": zz * R + yy, "pp": pp}

    def remote(src, dst, send, recv, device):
        return pltpu.make_async_remote_copy(src_ref=src, dst_ref=dst, send_sem=send, recv_sem=recv, device_id=device, device_id_type=MESH)

    barrier = pltpu.get_barrier_semaphore()
    for d in (1, 2, 3):
        for h in range(2):
            pl.semaphore_signal(barrier, inc=1, device_id=peer(h, 0, d), device_id_type=MESH)
            pl.semaphore_signal(barrier, inc=1, device_id=peer(h, 0, d, partner), device_id_type=MESH)

    @pl.when(stage > 0)
    def _():
        pl.semaphore_signal(barrier, inc=1, device_id={"pp": stage - 1}, device_id_type=MESH)

    @pl.when(stage < last)
    def _():
        pl.semaphore_signal(barrier, inc=1, device_id={"pp": stage + 1}, device_id_type=MESH)

    weight_copies = [
        pltpu.make_async_copy(wq_ref, wqkv.at[pl.ds(0, nqk)], w_sem.at[0]),
        pltpu.make_async_copy(wk_ref, wqkv.at[pl.ds(nqk, nqk)], w_sem.at[1]),
        pltpu.make_async_copy(wv_ref, wqkv.at[pl.ds(2 * nqk, nqk)], w_sem.at[2]),
        pltpu.make_async_copy(wup_ref, wup, w_sem.at[3]),
        pltpu.make_async_copy(wdown_ref, wcat.at[pl.ds(0, FF)], w_sem.at[4]),
        pltpu.make_async_copy(wo_ref, wcat.at[pl.ds(FF, nqk)], w_sem.at[5]),
    ]

    def input_copy(c):
        return pltpu.make_async_copy(x_ref.at[lax.div(c, 2), lax.rem(c, 2)], xg.at[c, z, y], in_sem.at[c])

    @pl.when(stage == 0)
    def _():
        for c in range(CHUNKS):
            input_copy(c).start()

    for cp in weight_copies:
        cp.start()

    pl.semaphore_wait(barrier, 12 + jnp.where(stage > 0, 1, 0) + jnp.where(stage < last, 1, 0))

    def hop_copy(c):
        return remote(ybuf.at[c], xg.at[c, z, y], hop_send.at[c], hop_recv.at[c], {"pp": lax.rem(stage + 1, pp_size)})

    def out_copy(c):
        return pltpu.make_async_copy(ybuf.at[c], out_ref.at[lax.div(c, 2), lax.rem(c, 2)], out_sem.at[c])

    def place(h, dv, du):
        v, u = home[h]
        return at(h, lax.rem(v + dv + R, R), lax.rem(u + du + R, R))

    def gathered(c, h, dv, du):
        zz, yy = place(h, dv, du)
        return xg.at[c, zz, yy, pl.ds(h * SUB, SUB), :]

    def partial_at(h, dv, du):
        zz, yy = place(h, dv, du)
        return part.at[zz, yy, pl.ds(h * SUB, SUB), :]

    def p1(c, h, d, incoming=False):
        view = gathered(c, h, 0, -d if incoming else 0)
        return remote(view, view, p1_send.at[h, d - 1], p1_recv.at[c, h, d - 1], peer(h, 0, d))

    def p2(c, h, side, k, incoming=False):
        view = gathered(c, h, ((-1, 1)[side] if incoming else 0), -k)
        return remote(view, view, p2_send.at[h, side, k], p2_recv.at[c, h, side, k], peer(h, (1, R - 1)[side], 0))

    def p3(c, h, k, incoming=False):
        side = SIDE[k]
        view = gathered(c, h, 2 if incoming else (-1, 1)[side] if k else 0, -k)
        return remote(view, view, p3_send.at[h, k], p3_recv.at[c, h, k], peer(h, (1, R - 1)[side] if k else 2, 0))

    def q1(c, h, k):
        return remote(partial_at(h, 2, -k), r1.at[c, h, k], q1_send.at[h, k], q1_recv.at[c, h, k], peer(h, (1, R - 1)[SIDE[k]], 0))

    def q2(c, h, side, k):
        return remote(partial_at(h, (1, -1)[side], -k), (r2 if side == 0 else r3).at[c, h, k], q2_send.at[h, side, k], q2_recv.at[c, h, side, k],
                      peer(h, (1, R - 1)[side], 0))

    def q3(c, h, k):
        return remote(mid.at[h, k], r4.at[c, h, k - 1], q3_send.at[h, k - 1], q3_recv.at[c, h, k - 1], peer(h, 0, R - k))

    def first_sends(c, direct=False):
        src_dev = stage + 1 if direct else stage
        copies = []
        for h in range(2):
            for i, (hh, dv, du) in enumerate([(h, 0, 1), (h, 0, 3), (1 - h, 1, 0), (1 - h, 3, 0), (h, 0, 2), (1 - h, 2, 0)]):
                dst = gathered(c, hh, 0, 0)
                src = ybuf.at[c, pl.ds(hh * SUB, SUB), :] if direct else dst
                if du:
                    send, recv = p1_send.at[hh, du - 1], p1_recv.at[c, hh, du - 1]
                elif dv == 2:
                    send, recv = p3_send.at[hh, 0], p3_recv.at[c, hh, 0]
                else:
                    send, recv = p2_send.at[hh, dv // 2, 0], p2_recv.at[c, hh, dv // 2, 0]
                copies.append(remote(src, dst, direct_send.at[c, h, i] if direct else send, recv, peer(hh, dv, du, src_dev)))
        return copies

    def norms(c, blocks):
        for h, dv, du in blocks:
            block = gathered(c, h, dv, du)
            zz, yy = place(h, dv, du)
            total = jnp.sum(block[...].astype(F32), axis=-1, keepdims=True)
            mean = total * (1.0 / D)
            dev = block[...].astype(F32) - mean
            var = jnp.sum(dev * dev, axis=-1, keepdims=True) * (1.0 / D)
            scale = lax.rsqrt(var + LN_EPS)
            unit = (block[...].astype(F32) - mean) * scale
            dst = pl.ds(pl.multiple_of(zz * GROUP + yy * BLK + h * SUB, SUB), SUB)
            ha[dst, :] = (unit * ln_ref[0:1, :] + ln_ref[1:2, :]).astype(BF16)
            hm[dst, :] = (unit * ln_ref[2:3, :] + ln_ref[3:4, :]).astype(BF16)

    def project(offs):
        toks = [pl.ds(pl.multiple_of(lax.rem(z + off, R) * GROUP, GROUP), GROUP) for off in offs]

        proj = nt_dot(wqkv[...], jnp.concatenate([ha[tok, :] for tok in toks], axis=0))
        for slot, tok in enumerate(toks):
            cols = proj[:, slot * GROUP:(slot + 1) * GROUP]
            cos, sin = cos_ref[:, tok], sin_ref[:, tok]

            def rope(row):
                first, second = cols[row:row + HH], cols[row + HH:row + HD]
                return jnp.concatenate([first * cos - second * sin, second * cos + first * sin], axis=0)

            for hd in range(HEADS):
                qv[pl.ds(hd * HD, HD), tok] = rope(hd * HD).astype(BF16)
                ks[hd, tok, :] = rope(nqk + hd * HD).T.astype(BF16)
            qv[pl.ds(nqk, nqk), tok] = cols[2 * nqk:].astype(BF16)

        for tok in toks:
            pre = nn_dot(hm[tok, :], wup[...])
            act[tok, 0:FF] = (0.5 * pre * (1.0 + lax.erf(pre * np.float32(0.5 ** 0.5)))).astype(BF16)

    def chunk(c, carry):
        with jax.named_scope("wait_in"):
            @pl.when(stage == 0)
            def _():
                input_copy(c).wait()

            @pl.when(stage > 0)
            def _():
                hop_copy(c).wait_recv()

            @pl.when((c > 0) & even)
            def _():
                pl.semaphore_wait(turn_sem, 1)

            @pl.when(even)
            def _():
                for cp in first_sends(c):
                    cp.start()

        with jax.named_scope("p1_wait"):
            for k in ORDER[1:]:
                for h in range(2):
                    p1(c, h, k, True).wait_recv()
                    for side in range(2):
                        p2(c, h, side, k).start()
        with jax.named_scope("norm_a"):
            norms(c, [(h, 0, -k) for k in ORDER for h in range(2)])
        with jax.named_scope("wait_b"):
            for h in (1, 0):
                for side in range(2):
                    p2(c, h, side, 0, True).wait_recv()
                p3(c, h, 0, True).wait_recv()
        with jax.named_scope("norm_b"):
            norms(c, [(h, dv, 0) for h in (1, 0) for dv in (-1, 1, 2)])
        def rest(k):
            for h in range(2):
                p2(c, h, 1 - SIDE[k], k, True).wait_recv()
            norms(c, [(h, dv, -k) for h in range(2) for dv in (-1, 1)])

        with jax.named_scope("forward"):
            for k in ORDER[1:]:
                for h in range(2):
                    p2(c, h, SIDE[k], k, True).wait_recv()
                    p3(c, h, k).start()
                if k != ORDER[-1]:
                    rest(k)

        @pl.when((c < CHUNKS - 1) & jnp.logical_not(even))
        def _():
            pl.semaphore_signal(turn_sem, inc=1, device_id={"pp": stage - 1}, device_id_type=MESH)

        @pl.when(c == 0)
        def _():
            for cp in weight_copies:
                cp.wait()

        with jax.named_scope("norm_c"):
            rest(ORDER[-1])
        with jax.named_scope("wait_e"):
            p3(c, 1, 1, True).wait_recv()
        with jax.named_scope("norm_e"):
            norms(c, [(1, 2, -1)])
        with jax.named_scope("proj03"):
            project((0, 3))
        with jax.named_scope("wait_f"):
            for h, k in LATE:
                p3(c, h, k, True).wait_recv()
        with jax.named_scope("norm_f"):
            norms(c, [(h, 2, -k) for h, k in LATE])
        with jax.named_scope("proj12"):
            project((1, 2))

        with jax.named_scope("attn"):
            for qb in range(2):
                toks = pl.ds(qb * 256, 256)
                nk = (qb + 1) * 256
                ctx = []
                for hd in range(HEADS):
                    scores = nn_dot(ks[hd, 0:nk, :], qv[pl.ds(hd * HD, HD), toks]) * (HD ** -0.5)
                    key_pos = lax.broadcasted_iota(jnp.int32, (nk, 256), 0)
                    query_pos = lax.broadcasted_iota(jnp.int32, (nk, 256), 1) + qb * 256
                    scores = jnp.where(query_pos >= key_pos, scores, -1e30)
                    top = jnp.max(scores, axis=0, keepdims=True)
                    probs = jnp.exp(scores - top)
                    total = jnp.sum(probs, axis=0, keepdims=True)
                    probs = (probs * (1.0 / total)).astype(BF16)
                    ctx.append(nn_dot(qv[pl.ds(nqk + hd * HD, HD), 0:nk], probs))
                act[toks, FF:ACT] = jnp.concatenate(ctx, axis=0).T.astype(BF16)

        def down(blocks):
            rows = []
            for h, dv, du in blocks:
                zz, yy = place(h, dv, du)
                rows.append(act[pl.ds(pl.multiple_of(zz * GROUP + yy * BLK + h * SUB, SUB), SUB), :])
            out = nn_dot(jnp.concatenate(rows, axis=0), wcat[...]).astype(BF16)
            for i, (h, dv, du) in enumerate(blocks):
                partial_at(h, dv, du)[...] = out[i * SUB:(i + 1) * SUB]

        with jax.named_scope("down"):
            down([(h, 2, -k) for h in range(2) for k in ORDER])
            for k in BACK:
                for h in range(2):
                    q1(c, h, k).start()
            for h in range(2):
                down([(h, dv, -k) for dv in (1, -1) for k in ORDER])
                for k in BACK:
                    for side in range(2):
                        if SIDE[k] != side:
                            q2(c, h, side, k).start()
            down([(h, 0, -k) for h in range(2) for k in ORDER])

        with jax.named_scope("rs_add"):
            for h, k in [(h, k) for k in BACK for h in range(2)]:
                side = SIDE[k]
                q1(c, h, k).wait_recv()
                mine = partial_at(h, (1, -1)[side], -k)
                mine[...] = (mine[...].astype(F32) + r1[c, h, k].astype(F32)).astype(BF16)
                q2(c, h, side, k).start()
        with jax.named_scope("rs_mid"):
            for h, k in [(h, k) for k in BACK for h in range(2)]:
                q2(c, h, 0, k).wait_recv()
                q2(c, h, 1, k).wait_recv()
                total = partial_at(h, 0, -k)[...].astype(F32) + r2[c, h, k].astype(F32) + r3[c, h, k].astype(F32)
                mid[h, k] = total.astype(BF16)
                if k:
                    q3(c, h, k).start()
        with jax.named_scope("rs_fin"):
            for h in range(2):
                rows = pl.ds(h * SUB, SUB)
                total = xg[c, z, y, rows, :].astype(F32) + mid[h, 0].astype(F32)
                for k in (1, 2, 3):
                    q3(c, h, k).wait_recv()
                    total += r4[c, h, k - 1].astype(F32)
                ybuf[c, rows, :] = total.astype(BF16)

        @pl.when(stage < last)
        def _():
            hop_copy(c).start()

        @pl.when(even)
        def _():
            for cp in first_sends(c, True):
                cp.start()

        out_copy(c).start()

        @pl.when(even)
        def _():
            for cp in first_sends(c):
                cp.wait_send()

        for h in range(2):
            for k in range(R):
                if k:
                    q3(c, h, k).wait_send()
                    p3(c, h, k).wait_send()
                for side in range(2):
                    if k:
                        p2(c, h, side, k).wait_send()
                    q2(c, h, side, k).wait_send()
                q1(c, h, k).wait_send()
        return carry

    lax.fori_loop(0, CHUNKS, chunk, 0)

    for c in range(CHUNKS):
        out_copy(c).wait()

        @pl.when(stage < last)
        def _():
            hop_copy(c).wait_send()

        @pl.when(even)
        def _():
            for cp in first_sends(c, True):
                cp.wait_send()


def solution(mesh):
    pp_size = mesh.shape["pp"]
    cos_tab, sin_tab = rope_tables()
    any_spec = pl.BlockSpec(memory_space=pl.ANY)
    vmem_spec = pl.BlockSpec(memory_space=pltpu.VMEM)
    dma = pltpu.SemaphoreType.DMA

    def body(x_in, ln_params, w_q, w_k, w_v, w_o, w_up, w_down):
        flat = HEADS * HD
        wq = jnp.transpose(w_q[0], (1, 2, 3, 0)).reshape(flat, D)
        wk = jnp.transpose(w_k[0], (1, 2, 0)).reshape(flat, D)
        wv = jnp.transpose(w_v[0], (1, 2, 0)).reshape(flat, D)
        wo = w_o[0].reshape(flat, D)
        out = pl.pallas_call(
            functools.partial(kernel, pp_size),
            out_shape=jax.ShapeDtypeStruct(x_in.shape, BF16),
            in_specs=[any_spec, vmem_spec] + [any_spec] * 6 + [vmem_spec, vmem_spec],
            out_specs=any_spec,
            scratch_shapes=[
                pltpu.VMEM((CHUNKS, R, R, BLK, D), BF16),
                pltpu.VMEM((QKV, D), BF16),
                pltpu.VMEM((D, FF), BF16),
                pltpu.VMEM((ACT, D), BF16),
                pltpu.VMEM((SEQ, D), BF16),
                pltpu.VMEM((SEQ, D), BF16),
                pltpu.VMEM((2 * flat, SEQ), BF16),
                pltpu.VMEM((HEADS, SEQ, HD), BF16),
                pltpu.VMEM((SEQ, ACT), BF16),
                pltpu.VMEM((R, R, BLK, D), BF16),
                pltpu.VMEM((CHUNKS, 2, R, SUB, D), BF16),
                pltpu.VMEM((CHUNKS, 2, R, SUB, D), BF16),
                pltpu.VMEM((CHUNKS, 2, R, SUB, D), BF16),
                pltpu.VMEM((2, R, SUB, D), BF16),
                pltpu.VMEM((CHUNKS, 2, R - 1, SUB, D), BF16),
                pltpu.VMEM((CHUNKS, BLK, D), BF16),
                dma((6,)), dma((CHUNKS,)), dma((CHUNKS,)), dma((CHUNKS,)), dma((CHUNKS,)),
                dma((2, 3)), dma((CHUNKS, 2, 3)), dma((2, 2, R)), dma((CHUNKS, 2, 2, R)), dma((2, R)), dma((CHUNKS, 2, R)),
                dma((2, R)), dma((CHUNKS, 2, R)), dma((2, 2, R)), dma((CHUNKS, 2, 2, R)), dma((2, 3)), dma((CHUNKS, 2, 3)),
                dma((CHUNKS, 2, 6)), pltpu.SemaphoreType.REGULAR,
            ],
            compiler_params=pltpu.CompilerParams(collective_id=1, has_side_effects=True, vmem_limit_bytes=62 * 2**20),
            name="pipeline",
        )(x_in, ln_params[0], wq, wk, wv, wo, w_up[0], w_down[0], jnp.asarray(cos_tab), jnp.asarray(sin_tab))
        return out[None]

    in_specs = (P(None, "dp", "tp", None), P("pp", None, None), P("pp", None, "tp", None, None), P("pp", None, "tp", None), P("pp", None, "tp", None), P("pp", "tp", None, None, None), P("pp", None, "tp"), P("pp", "tp", None))
    return jax.shard_map(body, mesh=mesh, in_specs=in_specs, out_specs=P("pp", None, "dp", "tp", None), check_vma=False)
```

```python
import functools

import jax
import jax.numpy as jnp
import numpy as np
from jax import lax
from jax.experimental import pallas as pl
from jax.experimental.pallas import tpu as pltpu
from jax.sharding import PartitionSpec as P

MESH = pl.DeviceIdType.MESH
LN_EPS = 1e-5
ROPE_BASE = 10000.0
F32, BF16 = jnp.float32, jnp.bfloat16

R = 4
BLK = 32
SEQ = R * R * BLK
D = 2560
SUB = BLK // 2
GROUP = R * BLK
ORDER = (0, 1, 3, 2)
BACK = (2, 1, 3, 0)
LATE = ((0, 1), (0, 3), (1, 3), (0, 2), (1, 2))
SIDE = (0, 1, 1, 0)
HEADS = 2
HD = 80
HH = HD // 2
FF = 640
QKV = 3 * HEADS * HD
ACT = FF + HEADS * HD
CHUNKS = 4


def rope_tables():
    positions = np.arange(SEQ, dtype=np.float32)
    inv_freq = (np.float32(ROPE_BASE) ** (np.float32(-2.0) * np.arange(HH, dtype=np.float32) / np.float32(HD))).astype(np.float32)
    angles = (inv_freq[:, None] * positions[None, :]).astype(np.float32)
    return np.cos(angles).astype(np.float32), np.sin(angles).astype(np.float32)


def nt_dot(a, b):
    return lax.dot_general(a, b, (((1,), (1,)), ((), ())), preferred_element_type=F32)


def nn_dot(a, b):
    return lax.dot_general(a, b, (((1,), (0,)), ((), ())), preferred_element_type=F32)


def kernel(pp_size, x_ref, ln_ref, wq_ref, wk_ref, wv_ref, wo_ref, wup_ref, wdown_ref, cos_ref, sin_ref, out_ref,
           xg, wqkv, wup, wcat, ha, hm, qv, ks, act, part, r1, r2, r3, mid, r4, ybuf,
           w_sem, in_sem, out_sem, hop_send, hop_recv, p1_send, p1_recv, p2_send, p2_recv, p3_send, p3_recv,
           q1_send, q1_recv, q2_send, q2_recv, q3_send, q3_recv, direct_send, turn_sem):
    tp = lax.axis_index("tp")
    stage = lax.axis_index("pp")
    z, y = lax.div(tp, R), lax.rem(tp, R)
    last = pp_size - 1
    even = lax.rem(stage, 2) == 0
    partner = stage + 1 - 2 * lax.rem(stage, 2)
    nqk = HEADS * HD

    home = ((z, y), (y, z))

    def at(h, v, u):
        return (v, u) if h == 0 else (u, v)

    def peer(h, dv, du, pp=stage):
        v, u = home[h]
        zz, yy = at(h, lax.rem(v + dv, R), lax.rem(u + du, R))
        return {"tp": zz * R + yy, "pp": pp}

    def remote(src, dst, send, recv, device):
        return pltpu.make_async_remote_copy(src_ref=src, dst_ref=dst, send_sem=send, recv_sem=recv, device_id=device, device_id_type=MESH)

    barrier = pltpu.get_barrier_semaphore()
    for d in (1, 2, 3):
        for h in range(2):
            pl.semaphore_signal(barrier, inc=1, device_id=peer(h, 0, d), device_id_type=MESH)
            pl.semaphore_signal(barrier, inc=1, device_id=peer(h, 0, d, partner), device_id_type=MESH)

    @pl.when(stage > 0)
    def _():
        pl.semaphore_signal(barrier, inc=1, device_id={"pp": stage - 1}, device_id_type=MESH)

    @pl.when(stage < last)
    def _():
        pl.semaphore_signal(barrier, inc=1, device_id={"pp": stage + 1}, device_id_type=MESH)

    weight_copies = [
        pltpu.make_async_copy(wq_ref, wqkv.at[pl.ds(0, nqk)], w_sem.at[0]),
        pltpu.make_async_copy(wk_ref, wqkv.at[pl.ds(nqk, nqk)], w_sem.at[1]),
        pltpu.make_async_copy(wv_ref, wqkv.at[pl.ds(2 * nqk, nqk)], w_sem.at[2]),
        pltpu.make_async_copy(wup_ref, wup, w_sem.at[3]),
        pltpu.make_async_copy(wdown_ref, wcat.at[pl.ds(0, FF)], w_sem.at[4]),
        pltpu.make_async_copy(wo_ref, wcat.at[pl.ds(FF, nqk)], w_sem.at[5]),
    ]

    def input_copy(c):
        return pltpu.make_async_copy(x_ref.at[lax.div(c, 2), lax.rem(c, 2)], xg.at[c, z, y], in_sem.at[c])

    @pl.when(stage == 0)
    def _():
        for c in range(CHUNKS):
            input_copy(c).start()

    for cp in weight_copies:
        cp.start()

    pl.semaphore_wait(barrier, 12 + jnp.where(stage > 0, 1, 0) + jnp.where(stage < last, 1, 0))

    def hop_copy(c):
        return remote(ybuf.at[c], xg.at[c, z, y], hop_send.at[c], hop_recv.at[c], {"pp": lax.rem(stage + 1, pp_size)})

    def out_copy(c):
        return pltpu.make_async_copy(ybuf.at[c], out_ref.at[lax.div(c, 2), lax.rem(c, 2)], out_sem.at[c])

    def place(h, dv, du):
        v, u = home[h]
        return at(h, lax.rem(v + dv + R, R), lax.rem(u + du + R, R))

    def gathered(c, h, dv, du):
        zz, yy = place(h, dv, du)
        return xg.at[c, zz, yy, pl.ds(h * SUB, SUB), :]

    def partial_at(h, dv, du):
        zz, yy = place(h, dv, du)
        return part.at[zz, yy, pl.ds(h * SUB, SUB), :]

    def p1(c, h, d, incoming=False):
        view = gathered(c, h, 0, -d if incoming else 0)
        return remote(view, view, p1_send.at[h, d - 1], p1_recv.at[c, h, d - 1], peer(h, 0, d))

    def p2(c, h, side, k, incoming=False):
        view = gathered(c, h, ((-1, 1)[side] if incoming else 0), -k)
        return remote(view, view, p2_send.at[h, side, k], p2_recv.at[c, h, side, k], peer(h, (1, R - 1)[side], 0))

    def p3(c, h, k, incoming=False):
        side = SIDE[k]
        view = gathered(c, h, 2 if incoming else (-1, 1)[side] if k else 0, -k)
        return remote(view, view, p3_send.at[h, k], p3_recv.at[c, h, k], peer(h, (1, R - 1)[side] if k else 2, 0))

    def q1(c, h, k):
        return remote(partial_at(h, 2, -k), r1.at[c, h, k], q1_send.at[h, k], q1_recv.at[c, h, k], peer(h, (1, R - 1)[SIDE[k]], 0))

    def q2(c, h, side, k):
        return remote(partial_at(h, (1, -1)[side], -k), (r2 if side == 0 else r3).at[c, h, k], q2_send.at[h, side, k], q2_recv.at[c, h, side, k],
                      peer(h, (1, R - 1)[side], 0))

    def q3(c, h, k):
        return remote(mid.at[h, k], r4.at[c, h, k - 1], q3_send.at[h, k - 1], q3_recv.at[c, h, k - 1], peer(h, 0, R - k))

    def first_sends(c, direct=False):
        src_dev = stage + 1 if direct else stage
        copies = []
        for h in range(2):
            for i, (hh, dv, du) in enumerate([(h, 0, 1), (h, 0, 3), (1 - h, 1, 0), (1 - h, 3, 0), (h, 0, 2), (1 - h, 2, 0)]):
                dst = gathered(c, hh, 0, 0)
                src = ybuf.at[c, pl.ds(hh * SUB, SUB), :] if direct else dst
                if du:
                    send, recv = p1_send.at[hh, du - 1], p1_recv.at[c, hh, du - 1]
                elif dv == 2:
                    send, recv = p3_send.at[hh, 0], p3_recv.at[c, hh, 0]
                else:
                    send, recv = p2_send.at[hh, dv // 2, 0], p2_recv.at[c, hh, dv // 2, 0]
                copies.append(remote(src, dst, direct_send.at[c, h, i] if direct else send, recv, peer(hh, dv, du, src_dev)))
        return copies

    def norms(c, blocks):
        for h, dv, du in blocks:
            block = gathered(c, h, dv, du)
            zz, yy = place(h, dv, du)
            total = jnp.sum(block[...].astype(F32), axis=-1, keepdims=True)
            mean = total * (1.0 / D)
            dev = block[...].astype(F32) - mean
            var = jnp.sum(dev * dev, axis=-1, keepdims=True) * (1.0 / D)
            scale = lax.rsqrt(var + LN_EPS)
            unit = (block[...].astype(F32) - mean) * scale
            dst = pl.ds(pl.multiple_of(zz * GROUP + yy * BLK + h * SUB, SUB), SUB)
            ha[dst, :] = (unit * ln_ref[0:1, :] + ln_ref[1:2, :]).astype(BF16)
            hm[dst, :] = (unit * ln_ref[2:3, :] + ln_ref[3:4, :]).astype(BF16)

    def project(offs):
        toks = [pl.ds(pl.multiple_of(lax.rem(z + off, R) * GROUP, GROUP), GROUP) for off in offs]

        proj = nt_dot(wqkv[...], jnp.concatenate([ha[tok, :] for tok in toks], axis=0))
        for slot, tok in enumerate(toks):
            cols = proj[:, slot * GROUP:(slot + 1) * GROUP]
            cos, sin = cos_ref[:, tok], sin_ref[:, tok]

            def rope(row):
                first, second = cols[row:row + HH], cols[row + HH:row + HD]
                return jnp.concatenate([first * cos - second * sin, second * cos + first * sin], axis=0)

            for hd in range(HEADS):
                qv[pl.ds(hd * HD, HD), tok] = rope(hd * HD).astype(BF16)
                ks[hd, tok, :] = rope(nqk + hd * HD).T.astype(BF16)
            qv[pl.ds(nqk, nqk), tok] = cols[2 * nqk:].astype(BF16)

        for tok in toks:
            pre = nn_dot(hm[tok, :], wup[...])
            act[tok, 0:FF] = (0.5 * pre * (1.0 + lax.erf(pre * np.float32(0.5 ** 0.5)))).astype(BF16)

    def chunk(c, carry):
        with jax.named_scope("wait_in"):
            @pl.when(stage == 0)
            def _():
                input_copy(c).wait()

            @pl.when(stage > 0)
            def _():
                hop_copy(c).wait_recv()

            @pl.when((c > 0) & even)
            def _():
                pl.semaphore_wait(turn_sem, 1)

            @pl.when(even)
            def _():
                for cp in first_sends(c):
                    cp.start()

        with jax.named_scope("p1_wait"):
            for k in ORDER[1:]:
                for h in range(2):
                    p1(c, h, k, True).wait_recv()
                    for side in range(2):
                        p2(c, h, side, k).start()
        with jax.named_scope("norm_a"):
            norms(c, [(h, 0, -k) for k in ORDER for h in range(2)])
        with jax.named_scope("wait_b"):
            for h in (1, 0):
                for side in range(2):
                    p2(c, h, side, 0, True).wait_recv()
                p3(c, h, 0, True).wait_recv()
        with jax.named_scope("norm_b"):
            norms(c, [(h, dv, 0) for h in (1, 0) for dv in (-1, 1, 2)])
        def rest(k):
            for h in range(2):
                p2(c, h, 1 - SIDE[k], k, True).wait_recv()
            norms(c, [(h, dv, -k) for h in range(2) for dv in (-1, 1)])

        with jax.named_scope("forward"):
            for k in ORDER[1:]:
                for h in range(2):
                    p2(c, h, SIDE[k], k, True).wait_recv()
                    p3(c, h, k).start()
                if k != ORDER[-1]:
                    rest(k)

        @pl.when((c < CHUNKS - 1) & jnp.logical_not(even))
        def _():
            pl.semaphore_signal(turn_sem, inc=1, device_id={"pp": stage - 1}, device_id_type=MESH)

        @pl.when(c == 0)
        def _():
            for cp in weight_copies:
                cp.wait()

        with jax.named_scope("norm_c"):
            rest(ORDER[-1])
        with jax.named_scope("wait_e"):
            p3(c, 1, 1, True).wait_recv()
        with jax.named_scope("norm_e"):
            norms(c, [(1, 2, -1)])
        with jax.named_scope("proj03"):
            project((0, 3))
        with jax.named_scope("wait_f"):
            for h, k in LATE:
                p3(c, h, k, True).wait_recv()
        with jax.named_scope("norm_f"):
            norms(c, [(h, 2, -k) for h, k in LATE])
        with jax.named_scope("proj12"):
            project((1, 2))

        with jax.named_scope("attn"):
            for qb in range(2):
                toks = pl.ds(qb * 256, 256)
                nk = (qb + 1) * 256
                key_pos = lax.broadcasted_iota(jnp.int32, (nk, 256), 0)
                query_pos = lax.broadcasted_iota(jnp.int32, (nk, 256), 1) + qb * 256
                allowed = query_pos >= key_pos
                scores = [nn_dot(ks[hd, 0:nk, :], qv[pl.ds(hd * HD, HD), toks]) * (HD ** -0.5) for hd in range(HEADS)]
                scores = [jnp.where(allowed, sc, -1e30) for sc in scores]
                probs = [jnp.exp(sc - jnp.max(sc, axis=0, keepdims=True)) for sc in scores]
                probs = [(pr * (1.0 / jnp.sum(pr, axis=0, keepdims=True))).astype(BF16) for pr in probs]
                ctx = [nn_dot(qv[pl.ds(nqk + hd * HD, HD), 0:nk], probs[hd]) for hd in range(HEADS)]
                act[toks, FF:ACT] = jnp.concatenate(ctx, axis=0).T.astype(BF16)

        def down(blocks):
            rows = []
            for h, dv, du in blocks:
                zz, yy = place(h, dv, du)
                rows.append(act[pl.ds(pl.multiple_of(zz * GROUP + yy * BLK + h * SUB, SUB), SUB), :])
            out = nn_dot(jnp.concatenate(rows, axis=0), wcat[...]).astype(BF16)
            for i, (h, dv, du) in enumerate(blocks):
                partial_at(h, dv, du)[...] = out[i * SUB:(i + 1) * SUB]

        with jax.named_scope("down"):
            down([(h, 2, -k) for h in range(2) for k in ORDER])
            for k in BACK:
                for h in range(2):
                    q1(c, h, k).start()
            for h in range(2):
                down([(h, dv, -k) for dv in (1, -1) for k in ORDER])
                for k in BACK:
                    for side in range(2):
                        if SIDE[k] != side:
                            q2(c, h, side, k).start()
            down([(h, 0, -k) for h in range(2) for k in ORDER])

        with jax.named_scope("rs_add"):
            for h, k in [(h, k) for k in BACK for h in range(2)]:
                side = SIDE[k]
                q1(c, h, k).wait_recv()
                mine = partial_at(h, (1, -1)[side], -k)
                mine[...] = (mine[...].astype(F32) + r1[c, h, k].astype(F32)).astype(BF16)
                q2(c, h, side, k).start()
        with jax.named_scope("rs_mid"):
            for h, k in [(h, k) for k in BACK for h in range(2)]:
                q2(c, h, 0, k).wait_recv()
                q2(c, h, 1, k).wait_recv()
                total = partial_at(h, 0, -k)[...].astype(F32) + r2[c, h, k].astype(F32) + r3[c, h, k].astype(F32)
                mid[h, k] = total.astype(BF16)
                if k:
                    q3(c, h, k).start()
        with jax.named_scope("rs_fin"):
            for h in range(2):
                rows = pl.ds(h * SUB, SUB)
                total = xg[c, z, y, rows, :].astype(F32) + mid[h, 0].astype(F32)
                for k in (1, 2, 3):
                    q3(c, h, k).wait_recv()
                    total += r4[c, h, k - 1].astype(F32)
                ybuf[c, rows, :] = total.astype(BF16)

        @pl.when(stage < last)
        def _():
            hop_copy(c).start()

        @pl.when(even)
        def _():
            for cp in first_sends(c, True):
                cp.start()

        out_copy(c).start()

        @pl.when(even)
        def _():
            for cp in first_sends(c):
                cp.wait_send()

        for h in range(2):
            for k in range(R):
                if k:
                    q3(c, h, k).wait_send()
                    p3(c, h, k).wait_send()
                for side in range(2):
                    if k:
                        p2(c, h, side, k).wait_send()
                    q2(c, h, side, k).wait_send()
                q1(c, h, k).wait_send()
        return carry

    lax.fori_loop(0, CHUNKS, chunk, 0)

    for c in range(CHUNKS):
        out_copy(c).wait()

        @pl.when(stage < last)
        def _():
            hop_copy(c).wait_send()

        @pl.when(even)
        def _():
            for cp in first_sends(c, True):
                cp.wait_send()


def solution(mesh):
    pp_size = mesh.shape["pp"]
    cos_tab, sin_tab = rope_tables()
    any_spec = pl.BlockSpec(memory_space=pl.ANY)
    vmem_spec = pl.BlockSpec(memory_space=pltpu.VMEM)
    dma = pltpu.SemaphoreType.DMA

    def body(x_in, ln_params, w_q, w_k, w_v, w_o, w_up, w_down):
        flat = HEADS * HD
        wq = jnp.transpose(w_q[0], (1, 2, 3, 0)).reshape(flat, D)
        wk = jnp.transpose(w_k[0], (1, 2, 0)).reshape(flat, D)
        wv = jnp.transpose(w_v[0], (1, 2, 0)).reshape(flat, D)
        wo = w_o[0].reshape(flat, D)
        out = pl.pallas_call(
            functools.partial(kernel, pp_size),
            out_shape=jax.ShapeDtypeStruct(x_in.shape, BF16),
            in_specs=[any_spec, vmem_spec] + [any_spec] * 6 + [vmem_spec, vmem_spec],
            out_specs=any_spec,
            scratch_shapes=[
                pltpu.VMEM((CHUNKS, R, R, BLK, D), BF16),
                pltpu.VMEM((QKV, D), BF16),
                pltpu.VMEM((D, FF), BF16),
                pltpu.VMEM((ACT, D), BF16),
                pltpu.VMEM((SEQ, D), BF16),
                pltpu.VMEM((SEQ, D), BF16),
                pltpu.VMEM((2 * flat, SEQ), BF16),
                pltpu.VMEM((HEADS, SEQ, HD), BF16),
                pltpu.VMEM((SEQ, ACT), BF16),
                pltpu.VMEM((R, R, BLK, D), BF16),
                pltpu.VMEM((CHUNKS, 2, R, SUB, D), BF16),
                pltpu.VMEM((CHUNKS, 2, R, SUB, D), BF16),
                pltpu.VMEM((CHUNKS, 2, R, SUB, D), BF16),
                pltpu.VMEM((2, R, SUB, D), BF16),
                pltpu.VMEM((CHUNKS, 2, R - 1, SUB, D), BF16),
                pltpu.VMEM((CHUNKS, BLK, D), BF16),
                dma((6,)), dma((CHUNKS,)), dma((CHUNKS,)), dma((CHUNKS,)), dma((CHUNKS,)),
                dma((2, 3)), dma((CHUNKS, 2, 3)), dma((2, 2, R)), dma((CHUNKS, 2, 2, R)), dma((2, R)), dma((CHUNKS, 2, R)),
                dma((2, R)), dma((CHUNKS, 2, R)), dma((2, 2, R)), dma((CHUNKS, 2, 2, R)), dma((2, 3)), dma((CHUNKS, 2, 3)),
                dma((CHUNKS, 2, 6)), pltpu.SemaphoreType.REGULAR,
            ],
            compiler_params=pltpu.CompilerParams(collective_id=1, has_side_effects=True, vmem_limit_bytes=62 * 2**20),
            name="pipeline",
        )(x_in, ln_params[0], wq, wk, wv, wo, w_up[0], w_down[0], jnp.asarray(cos_tab), jnp.asarray(sin_tab))
        return out[None]

    in_specs = (P(None, "dp", "tp", None), P("pp", None, None), P("pp", None, "tp", None, None), P("pp", None, "tp", None), P("pp", None, "tp", None), P("pp", "tp", None, None, None), P("pp", None, "tp"), P("pp", "tp", None))
    return jax.shard_map(body, mesh=mesh, in_specs=in_specs, out_specs=P("pp", None, "dp", "tp", None), check_vma=False)
```
